256 devices in a mesh: rep: 2 (over core), dp: 128 (over x, y, z).
Axes of the slice: x: 4, y: 4, z: 8, core: 2. Of those that a mesh axis runs over, the one named last changes fastest.
Arguments:
- x: bfloat16 [256, 2048, 896], P(('rep', 'dp')), parts along dimension 0
- dy: bfloat16 [256, 2048, 896], P(('rep', 'dp')), parts along dimension 0
- w_gate: bfloat16 [2, 896, 2304], replicated
- w_up: bfloat16 [2, 896, 2304], replicated
- w_down: bfloat16 [2, 2304, 896], replicated
- m_w_gate: float32 [2, 896, 2304], replicated
- m_w_up: float32 [2, 896, 2304], replicated
- m_w_down: float32 [2, 2304, 896], replicated
- v_w_gate: float32 [2, 896, 2304], replicated
- v_w_up: float32 [2, 896, 2304], replicated
- v_w_down: float32 [2, 2304, 896], replicated
Outputs:
- output 1: bfloat16 [4, 896, 2304], P('rep'), parts along dimension 0
- output 2: bfloat16 [4, 896, 2304], P('rep'), parts along dimension 0
- output 3: bfloat16 [4, 2304, 896], P('rep'), parts along dimension 0
- output 4: float32 [4, 896, 2304], P('rep'), parts along dimension 0
- output 5: float32 [4, 896, 2304], P('rep'), parts along dimension 0
- output 6: float32 [4, 2304, 896], P('rep'), parts along dimension 0
- output 7: float32 [4, 896, 2304], P('rep'), parts along dimension 0
- output 8: float32 [4, 896, 2304], P('rep'), parts along dimension 0
- output 9: float32 [4, 2304, 896], P('rep'), parts along dimension 0
There are 2 independent parts. The reference program is written for one: setup_inputs(seed, part) draws one part's arguments, and reference() takes and returns one part's arrays. A program takes and returns all parts, laid end to end along the dimension named above; an argument that names none is the same for every part.
All inputs are finite; a program needn't handle non-finite values.
Results may differ from the reference program's by a relative error of at most 0.022.
Values are sent between devices in bfloat16 or wider.
A program may use at most 768 MiB of HBM per device.

```python
import jax
import jax.numpy as jnp
from jax import lax

SEQUENCES = 128
TOKENS = 2048
D = 896
FF = 2304
LAYERS = 2
NAMES = ("w_gate", "w_up", "w_down")
SHAPES = {"w_gate": (LAYERS, D, FF), "w_up": (LAYERS, D, FF), "w_down": (LAYERS, FF, D)}


def bump(key, n, height):
    away = (jnp.arange(n, dtype=jnp.int32) - jax.random.randint(key, (), 0, n, jnp.int32)) % n
    return jnp.where(away < n // 8, height, 1.0)


def together(key, own, strength):
    shared = jax.random.normal(key, own.shape[1:], jnp.float32)
    return (own + strength * shared) * lax.rsqrt(1 + strength * strength)


def setup_inputs(seed: int = 0, part: int = 0) -> dict:
    kx, kdy, ka, kb, kz, kf, kh, kl, *keys = jax.random.split(jax.random.key(seed), 8 + 3 * len(NAMES))
    kx, kdy, ka, kb = (jax.random.fold_in(k, part) for k in (kx, kdy, ka, kb))
    kw, km, kv = (keys[i::3] for i in range(3))
    shape = (SEQUENCES, TOKENS, D)
    much_x, much_dy = jax.random.uniform(kz, (2,), jnp.float32, 0.0, 1.0)
    loud = 2.0 ** jax.random.uniform(jax.random.fold_in(kz, 1), (), jnp.float32, -1.0, 2.0)
    layers = 2.0 ** jax.random.uniform(kl, (LAYERS, 1, 1), jnp.float32, -1.0, 1.0)
    x = together(ka, jax.random.normal(kx, shape, jnp.float32), much_x) * bump(kf, D, 4.0)
    dy = together(kb, jax.random.normal(kdy, shape, jnp.float32), much_dy)
    drawn = {"x": x.astype(jnp.bfloat16), "dy": (loud * dy * (SEQUENCES * TOKENS) ** -0.5).astype(jnp.bfloat16)}
    for key, name in zip(kw, NAMES, strict=True):
        w = jax.random.normal(key, SHAPES[name], jnp.float32) * SHAPES[name][1] ** -0.5
        drawn[name] = (w * {"w_gate": 1.0, "w_up": bump(kh, FF, 4.0), "w_down": layers}[name]).astype(jnp.bfloat16)
    for key, name in zip(km, NAMES, strict=True):
        drawn[f"m_{name}"] = 0.1 * jax.random.normal(key, SHAPES[name], jnp.float32)
    for key, name in zip(kv, NAMES, strict=True):
        drawn[f"v_{name}"] = jax.random.uniform(key, SHAPES[name], jnp.float32, 0.005, 0.015)
    return drawn


def matmul(a, w):
    return jnp.dot(a, w, preferred_element_type=jnp.float32).astype(jnp.bfloat16)


def normed(h):
    wide = h.astype(jnp.float32)
    scale = lax.rsqrt(jnp.mean(wide**2, -1, keepdims=True) + 1e-6)
    return (wide * scale).astype(jnp.bfloat16)


def layer(h, w):
    a = normed(h)
    gate = jnp.dot(a, w["w_gate"], preferred_element_type=jnp.float32)
    up = jnp.dot(a, w["w_up"], preferred_element_type=jnp.float32)
    return h + matmul((jax.nn.silu(gate) * up).astype(jnp.bfloat16), w["w_down"])


def adamw(w, m, v, g):
    m = 0.9 * m + 0.1 * g
    v = 0.95 * v + 0.05 * g * g
    step = m * lax.rsqrt(v + 1e-8) + 0.1 * w
    return (w - 0.02 * step).astype(jnp.bfloat16), m, v


def clipped(gradients, sum_of_squares, count):
    factor = jnp.minimum(1.0, 0.5 * lax.rsqrt(sum_of_squares / count + 1e-30))
    return [g * factor for g in gradients]


def stack(weights, h):
    return lax.scan(lambda h, w: (layer(h, w), None), h, weights)[0]


def reference(x, dy, w_gate, w_up, w_down, m_w_gate, m_w_up, m_w_down, v_w_gate, v_w_up, v_w_down):
    weights = dict(zip(NAMES, (w_gate, w_up, w_down), strict=True))

    def take(so_far, sequence):
        h, by_y = sequence
        _, back = jax.vjp(lambda w: stack(w, h), weights)
        return jax.tree.map(lambda total, term: total + term.astype(jnp.float32), so_far, back(by_y)[0]), None

    none_yet = {name: jnp.zeros(w.shape, jnp.float32) for name, w in weights.items()}
    by_weights, _ = lax.scan(take, none_yet, (x, dy))
    gradients = [by_weights[name].astype(jnp.bfloat16).astype(jnp.float32) for name in NAMES]
    gradients = clipped(gradients, sum(jnp.sum(g * g) for g in gradients), sum(g.size for g in gradients))
    new = [
        adamw(w.astype(jnp.float32), m, v, g)
        for w, m, v, g in zip((w_gate, w_up, w_down), (m_w_gate, m_w_up, m_w_down), (v_w_gate, v_w_up, v_w_down), gradients, strict=True)
    ]
    return tuple(one[which] for which in range(3) for one in new)
```

```python
import functools

import jax
import jax.numpy as jnp
from jax import lax
from jax.experimental import pallas as pl
from jax.experimental.pallas import tpu as pltpu
from jax.sharding import PartitionSpec as P

NAMES = ("w_gate", "w_up", "w_down")
BF, F32 = jnp.bfloat16, jnp.float32
MESH = pl.DeviceIdType.MESH
SIZES = {"x": 4, "y": 4, "z": 8}
AXES = ("x", "y", "z")
LANES = 128
SHARD = 128
ORDERS = (("z", "x", "y"), ("x", "y", "z"), ("y", "x", "z"))
ROWS = ((48, 48, 32), (48, 32, 48), (32, 48, 48))


def colour(k, c):
    rows = ROWS[k % 3]
    return sum(rows[:c]), rows[c]


def steps_of(c):
    return [(p, axis, s, SIZES[axis] // 2) for p, axis in enumerate(ORDERS[c]) for s in range(1, SIZES[axis] // 2 + 1)]


def order_of_steps(count, ready, busy):
    rate, latency, serve = 46.0e3, 2.2, 0.35
    free = {axis: 0.0 for axis in AXES}
    arrival, position = {}, {}
    now, served = 0.0, []

    def size(k, c, at):
        phase, axis, s, last = steps_of(c)[at]
        owned = SHARD * 128 * LANES * 2 * colour(k, c)[1] // 128
        for done in ORDERS[c][: phase + 1]:
            owned //= SIZES[done]
        return owned // 2 if s == 1 else owned

    def send(k, c, at):
        axis = steps_of(c)[at][1]
        begin = max(now, free[axis])
        free[axis] = begin + size(k, c, at) / rate
        arrival[k, c] = free[axis] + latency
        position[k, c] = at

    waiting = [(k, c) for k in range(count) for c in range(3)]
    while waiting or arrival:
        choices = [(arrival[kc], kc[0], 1, kc) for kc in arrival]
        for c in range(3):
            first = next((kc for kc in waiting if kc[1] == c), None)
            if first is not None:
                axis = ORDERS[c][0]
                choices.append((max(ready[first[0]], free[axis] - 2.0), first[0], 0, first))
        when, _, kind, kc = min(choices)
        now = max(now, when)
        for begin, end in busy:
            if begin <= now < end:
                now = end
        now += serve
        served.append((now, kc))
        if kind == 0:
            waiting.remove(kc)
            send(*kc, 0)
        elif position[kc] + 1 < len(steps_of(kc[1])):
            send(*kc, position[kc] + 1)
        else:
            del arrival[kc]
    return served


def recv_shapes(count):
    shapes = []
    for k in range(count):
        for c in range(3):
            for phase in range(3):
                axes = ORDERS[c]
                left = tuple(SIZES[a] for a in AXES if a not in axes[: phase + 1])
                shapes.append(pltpu.VMEM((SIZES[axes[phase]] - 1, *left, colour(k, c)[1], LANES), BF))
    return shapes


def here():
    d = lax.axis_index("dp")
    return {"x": d // 32, "y": (d // 8) % 4, "z": d % 8}


def device(at, axis, value):
    at = dict(at, **{axis: value})
    return {"dp": (at["x"] * 4 + at["y"]) * 8 + at["z"]}


def shifted(at, axis, by):
    n = SIZES[axis]
    return (at[axis] + (by % n)) % n


def meet(at):
    barrier = pltpu.get_barrier_semaphore()
    peers = [(axis, by) for axis in AXES for by in range(1, SIZES[axis])]
    for axis, by in peers:
        pl.semaphore_signal(barrier, inc=1, device_id=device(at, axis, shifted(at, axis, by)), device_id_type=MESH)
    pl.semaphore_wait(barrier, len(peers))


def stream(k, c, at, own, recv, send_sem, recv_sem, finish):
    first, rows = colour(k, c)
    axes = ORDERS[c]
    sent = [None, None]

    def part(index, axis, half):
        place, halved = [], half is None
        for a in AXES:
            if a in index:
                place.append(index[a])
            elif not halved:
                n = SIZES[a] // 2
                place.append(pl.ds(half * n, n))
                halved = True
            else:
                place.append(slice(None))
        begin, size = first, rows
        if not halved:
            one = (rows // 2 + 15) // 16 * 16
            begin, size = (first, one) if half == 0 else (first + one, rows - one)
        return tuple(place) + (pl.ds(begin, size), slice(None))

    def slot(number, index, half):
        place, halved = [number], half is None
        for a in AXES:
            if a not in index:
                if not halved:
                    n = SIZES[a] // 2
                    place.append(pl.ds(half * n, n))
                    halved = True
                else:
                    place.append(slice(None))
        if not halved:
            one = (rows // 2 + 15) // 16 * 16
            place.append(pl.ds(0, one) if half == 0 else pl.ds(one, rows - one))
        else:
            place.append(slice(None))
        return tuple(place) + (slice(None),)

    def add(target, buffers, total=None):
        def body(i, carry):
            place = (i,) if i is not None else (...,)
            value = target[place].astype(F32)
            for b in buffers:
                value = value + b[place].astype(F32)
            target[place] = value.astype(BF)
            return carry

        if len(target.shape) == 4:
            lax.fori_loop(0, target.shape[0], body, 0)
        else:
            body(None, 0)

    fixed = {}
    for phase, axis in enumerate(axes):
        n = SIZES[axis]
        h = n // 2
        buffer = recv[(k * 3 + c) * 3 + phase]
        base = sum(SIZES[a] // 2 for a in axes[:phase])
        ends = (device(at, axis, shifted(at, axis, 1)), device(at, axis, shifted(at, axis, -1)))

        def owner(by):
            return dict(fixed, **{axis: shifted(at, axis, by)})

        def slots(s, d):
            index = owner(0)
            return slot(0 if s == 1 else 2 * s - 3 + d, index, d if s == 1 else None)

        def copy(s, d):
            by = (h - s + 1) * (1, -1)[d]
            half = d if s == 1 else None
            return pltpu.make_async_remote_copy(
                src_ref=own.at[part(owner(by), axis, half)],
                dst_ref=buffer.at[slots(s, d)],
                send_sem=send_sem.at[k, c, d],
                recv_sem=recv_sem.at[k, c, base + s - 1, d],
                device_id=ends[d],
                device_id_type=MESH,
            )

        def go(s):
            for d in range(2):
                if sent[d] is not None:
                    sent[d].wait_send()
                sent[d] = copy(s, d)
                sent[d].start()

        go(1)
        yield
        for s in range(1, h + 1):
            for d in range(2):
                copy(s, d).wait_recv()
            if s < h:
                for d in range(2):
                    by = (h - s) * (1, -1)[d]
                    half = d if s == 1 else None
                    index = part(owner(by), axis, None)
                    index = part(owner(by), axis, half)
                    add(own.at[index], [buffer.at[slots(s, d)]])
                go(s + 1)
                yield
            else:
                if h == 1:
                    raise ValueError
                add(own.at[part(owner(0), axis, None)], [buffer.at[slots(s, d)] for d in range(2)])
        fixed = owner(0)
    for d in range(2):
        sent[d].wait_send()
    finish(k, c, own.at[part(fixed, axes[-1], None)])


def total_of(at, local, boxes, send_sem, recv_sem):
    number = 0
    for axis in ("z", "x", "y"):
        n = SIZES[axis]
        box = boxes[axis]
        box[at[axis]] = local
        copies = []
        for by in range(1, n):
            copies.append(
                pltpu.make_async_remote_copy(
                    src_ref=box.at[at[axis]],
                    dst_ref=box.at[at[axis]],
                    send_sem=send_sem.at[number],
                    recv_sem=recv_sem.at[number],
                    device_id=device(at, axis, shifted(at, axis, by)),
                    device_id_type=MESH,
                )
            )
            number += 1
        for one in copies:
            one.start()
        for one in copies:
            one.wait()
        local = box[0]
        for i in range(1, n):
            local = local + box[i]
    return local


def reduce_kernel(count, last, *refs):
    grads, refs = refs[:count], refs[count:]
    if last:
        before_ref, refs = refs[0], refs[1:]
    shard_ref, total_ref, own, refs = refs[0], refs[1], refs[2], refs[3:]
    recv, refs = refs[: 9 * count], refs[9 * count :]
    box_x, box_y, box_z, squares, load_sem, send_sem, recv_sem, sum_send, sum_recv = refs
    at = here()
    loads = [pltpu.make_async_copy(grads[k], own.at[k], load_sem.at[k]) for k in range(count)]
    for one in loads:
        one.start()
    meet(at)
    squares[...] = before_ref[...] if last else jnp.zeros_like(squares)

    def finish(k, c, region):
        first, rows = colour(k, c)
        value = region[...]
        shard_ref[k, pl.ds(first, rows), :] = value
        wide = value.astype(F32)
        squares[...] += jnp.sum((wide * wide).reshape(rows // 8, 8, LANES), axis=0)

    streams = {}
    loaded = set()
    for _, (k, c) in order_of_steps(count, [2.0 * k for k in range(count)], []):
        if k not in loaded:
            loads[k].wait()
            loaded.add(k)
        if (k, c) not in streams:
            streams[k, c] = stream(k, c, at, own.at[k], recv, send_sem, recv_sem, finish)
        next(streams[k, c], None)
    value = squares[...]
    if last:
        value = total_of(at, value, {"x": box_x, "y": box_y, "z": box_z}, sum_send, sum_recv)
    total_ref[...] = value


def reduced(grads, before=None):
    count, last = len(grads), before is not None
    sent = sum(g.size for g in grads) * 2
    return pl.pallas_call(
        functools.partial(reduce_kernel, count, last),
        out_shape=(jax.ShapeDtypeStruct((count, SHARD, LANES), BF), jax.ShapeDtypeStruct((8, LANES), F32)),
        in_specs=[pl.BlockSpec(memory_space=pltpu.HBM)] * count + [pl.BlockSpec(memory_space=pltpu.VMEM)] * last,
        out_specs=[pl.BlockSpec(memory_space=pltpu.VMEM)] * 2,
        scratch_shapes=[
            pltpu.VMEM((count, 4, 4, 8, SHARD, LANES), BF),
            *recv_shapes(count),
            pltpu.VMEM((4, 8, LANES), F32),
            pltpu.VMEM((4, 8, LANES), F32),
            pltpu.VMEM((8, 8, LANES), F32),
            pltpu.VMEM((8, LANES), F32),
            pltpu.SemaphoreType.DMA((count,)),
            pltpu.SemaphoreType.DMA((count, 3, 2)),
            pltpu.SemaphoreType.DMA((count, 3, 8, 2)),
            pltpu.SemaphoreType.DMA((13,)),
            pltpu.SemaphoreType.DMA((13,)),
        ],
        compiler_params=pltpu.CompilerParams(collective_id=int(last), has_side_effects=True, vmem_limit_bytes=66_000_000),
        cost_estimate=pl.CostEstimate(flops=sent * 1000, bytes_accessed=sent, transcendentals=0),
        name="reduce",
    )(*grads, *([before] if last else []))


PANEL = 256


def adamw_kernel(down, aliased, factor_ref, g_ref, w_ref, m_ref, v_ref, *refs):
    wo_ref, mo_ref, vo_ref = refs[3 * aliased :]
    factor = factor_ref[0]

    def one(g, place):
        g = g.astype(F32) * factor
        w = w_ref[place].astype(F32)
        m = 0.9 * m_ref[place] + 0.1 * g
        v = 0.95 * v_ref[place] + 0.05 * g * g
        step = m * lax.rsqrt(v + 1e-8) + 0.1 * w
        wo_ref[place] = (w - 0.02 * step).astype(BF)
        mo_ref[place] = m
        vo_ref[place] = v

    for half in range(PANEL // LANES):
        lanes = pl.ds(half * LANES, LANES)

        def body(i, carry):
            rows = pl.ds(pl.multiple_of(i * 128, 128), 128)
            g = g_ref[pl.ds(pl.multiple_of(half * 896 + i * 128, 128), 128), :]
            if down:
                one(g.astype(F32).T, (lanes, rows))
            else:
                one(g, (rows, lanes))
            return carry

        if down:
            for i in range(7):
                one(g_ref[pl.ds(half * 896 + i * 128, 128), :].astype(F32).T, (lanes, pl.ds(i * 128, 128)))
        else:
            lax.fori_loop(0, 7, body, 0)


def adamw(layer, down, factor, g, w, m, v, before):
    block = (None, PANEL, 896) if down else (None, 896, PANEL)
    at = (lambda p: (layer, p, 0)) if down else (lambda p: (layer, 0, p))
    spec = pl.BlockSpec(block, at)
    aliased = before is not None
    extra = list(before) if aliased else []
    size = w.size // 2
    return pl.pallas_call(
        functools.partial(adamw_kernel, down, aliased),
        grid=(2304 // PANEL,),
        out_shape=(jax.ShapeDtypeStruct(w.shape, BF), jax.ShapeDtypeStruct(w.shape, F32), jax.ShapeDtypeStruct(w.shape, F32)),
        in_specs=[
            pl.BlockSpec(memory_space=pltpu.SMEM),
            pl.BlockSpec((7 * PANEL, LANES), lambda p: (p, 0)),
            spec,
            spec,
            spec,
            *[pl.BlockSpec(memory_space=pltpu.HBM)] * len(extra),
        ],
        out_specs=[spec] * 3,
        input_output_aliases={5 + i: i for i in range(3)} if aliased else {},
        compiler_params=pltpu.CompilerParams(vmem_limit_bytes=66_000_000, dimension_semantics=("arbitrary",)),
        cost_estimate=pl.CostEstimate(flops=size * 200, bytes_accessed=size * 22, transcendentals=size),
        name="adamw",
    )(factor, g, w, m, v, *extra)


def matmul(a, w):
    return jnp.dot(a, w, preferred_element_type=jnp.float32).astype(jnp.bfloat16)


def normed(h):
    wide = h.astype(jnp.float32)
    scale = lax.rsqrt(jnp.mean(wide**2, -1, keepdims=True) + 1e-6)
    return (wide * scale).astype(jnp.bfloat16)


def layer(h, w):
    a = normed(h)
    gate = jnp.dot(a, w["w_gate"], preferred_element_type=jnp.float32)
    up = jnp.dot(a, w["w_up"], preferred_element_type=jnp.float32)
    return h + matmul((jax.nn.silu(gate) * up).astype(jnp.bfloat16), w["w_down"])


def as_shards(g):
    g = g.reshape(896, 18, LANES).transpose(1, 0, 2).reshape(18 * 896, LANES)
    g = jnp.concatenate([g, jnp.zeros((128 * SHARD - 18 * 896, LANES), BF)])
    return g.reshape(4, 4, 8, SHARD, LANES)


def solution(mesh):
    def step(x, dy, *arrays):
        weights, m, v = (arrays[i : i + 3] for i in (0, 3, 6))
        layers = weights[0].shape[0]
        h, kept = x[0], []
        for number in range(layers):
            kept.append(h)
            h = layer(h, {name: w[number] for name, w in zip(NAMES, weights, strict=True)})
        by_h, grads = dy[0], []
        for number in reversed(range(layers)):
            _, back = jax.vjp(lambda w, h: layer(h, w), {name: w[number] for name, w in zip(NAMES, weights, strict=True)}, kept[number])
            by_w, by_h = back(by_h)
            grads += [as_shards(by_w["w_down"].T), as_shards(by_w["w_gate"]), as_shards(by_w["w_up"])]
        first, squares = reduced(grads[:3])
        second, squares = reduced(grads[3:], squares)
        shards = [first[0], first[1], first[2], second[0], second[1], second[2]]
        total = jnp.sum(squares)
        factor = jnp.minimum(1.0, 0.5 * lax.rsqrt(total / (6 * 896 * 2304) + 1e-30)).reshape(1)
        new = {}
        for k, (number, name) in enumerate((n, name) for n in (1, 0) for name in ("w_down", "w_gate", "w_up")):
            g = lax.all_gather(shards[k], "dp", axis=0, tiled=True)
            i = NAMES.index(name)
            new[name] = adamw(number, name == "w_down", factor, g, weights[i], m[i], v[i], new.get(name))
        return tuple(new[name][which] for which in range(3) for name in NAMES)

    return jax.shard_map(
        step,
        mesh=mesh,
        in_specs=(P(("rep", "dp"), None, None),) * 2 + (P(None, None, None),) * 9,
        out_specs=(P("rep", None, None),) * 9,
        check_vma=False,
    )
```

```python
import functools

import jax
import jax.numpy as jnp
from jax import lax
from jax.experimental import pallas as pl
from jax.experimental.pallas import tpu as pltpu
from jax.sharding import PartitionSpec as P

BF, F32 = jnp.bfloat16, jnp.float32
MESH = pl.DeviceIdType.MESH
SIZES = {"x": 4, "y": 4, "z": 8}
AXES = ("x", "y", "z")
LANES = 128
SHARD = 128
D, FF, TOKENS = 896, 2304, 2048
PANEL = 256
PANELS = FF // PANEL
LIMIT = 66_900_000
ORDERS = (("z", "x", "y"), ("x", "y", "z"), ("y", "x", "z"))
ROWS = ((48, 48, 32), (48, 32, 48), (32, 48, 48))


def colour(j, c):
    return sum(ROWS[j][:c]), ROWS[j][c]


def here():
    d = lax.axis_index("dp")
    return {"x": d // 32, "y": (d // 8) % 4, "z": d % 8}


def device(at, axis, value):
    at = dict(at, **{axis: value})
    return {"dp": (at["x"] * 4 + at["y"]) * 8 + at["z"]}


def shifted(at, axis, by):
    n = SIZES[axis]
    return (at[axis] + (by % n)) % n


def meet(at):
    barrier = pltpu.get_barrier_semaphore()
    peers = [(axis, by) for axis in AXES for by in range(1, SIZES[axis])]
    for axis, by in peers:
        pl.semaphore_signal(barrier, inc=1, device_id=device(at, axis, shifted(at, axis, by)), device_id_type=MESH)
    pl.semaphore_wait(barrier, len(peers))


def place_of(fixed, half, first, rows):
    place, halved = [], half is None
    for a in AXES:
        if a in fixed:
            place.append(fixed[a])
        elif not halved:
            n = SIZES[a] // 2
            place.append(pl.ds(half * n, n))
            halved = True
        else:
            place.append(slice(None))
    begin, size = first, rows
    if not halved:
        one = (rows // 2 + 15) // 16 * 16
        begin, size = (first, one) if half == 0 else (first + one, rows - one)
    return tuple(place) + (pl.ds(begin, size), slice(None))


RATE, LATENCY, SERVE = 45.0e3, 2.2, 0.3


def bytes_of(j, c, phase, part):
    size = SHARD * SHARD * LANES * 2 * ROWS[j][c] // SHARD
    for axis in ORDERS[c][: phase + 1]:
        size //= SIZES[axis]
    return size * part


def scatter_steps(j, c):
    out = []
    for phase, axis in enumerate(ORDERS[c]):
        for s in range(1, SIZES[axis] // 2 + 1):
            out.append((axis, bytes_of(j, c, phase, 0.5 if s == 1 else 1)))
    return out


def gather_steps(j, c):
    out = []
    for phase, axis in reversed(list(enumerate(ORDERS[c]))):
        h = SIZES[axis] // 2
        for s in range(1, h + 1):
            out.append((axis, 2 * bytes_of(j, c, phase, 0.5 if s == h else 1)))
    return out


def serve_order(streams, ready, panels, panel_time):
    free = {axis: 0.0 for axis in AXES}
    arrival, position = {}, {}
    now, done, out = 0.0, 0, []
    waiting = list(streams)

    def send(key, at):
        axis, size = streams[key][at]
        free[axis] = max(now, free[axis]) + size / RATE
        arrival[key], position[key] = free[axis] + LATENCY, at

    while waiting or arrival or done < panels:
        choices = sorted((t, key) for key, t in arrival.items())
        start = next((key for key in waiting if ready[key] <= done and free[streams[key][0][0]] < now + 3.0), None)
        if start is not None:
            now += SERVE
            out.append((now, start))
            waiting.remove(start)
            send(start, 0)
        elif choices and choices[0][0] <= now:
            key = choices[0][1]
            now += SERVE
            out.append((now, key))
            del arrival[key]
            if position[key] + 1 < len(streams[key]):
                send(key, position[key] + 1)
        elif done < panels:
            now += panel_time
            out.append((now, done))
            done += 1
        else:
            later = [choices[0][0]] if choices else []
            later += [free[streams[key][0][0]] - 3.0 for key in waiting]
            now = max(now + 0.01, min(later))
    return out


TB = 256


def dot(a, b):
    return lax.dot_general(a, b, (((1,), (0,)), ((), ())), preferred_element_type=F32)


def dot_t(a, b):
    return lax.dot_general(a, b, (((1,), (1,)), ((), ())), preferred_element_type=F32)


def rows_kernel(x_ref, dy_ref, wg_ref, wu_ref, wd_ref, xt_ref, ys_ref, wg, wu, wd, gate0, up0, a_buf, h_buf, load_sem):
    first = pl.program_id(0) == 0
    loads = {
        (name, layer): pltpu.make_async_copy(ref.at[layer], buf.at[layer], load_sem.at[n, layer])
        for n, (name, ref, buf) in enumerate((("g", wg_ref, wg), ("u", wu_ref, wu), ("d", wd_ref, wd)))
        for layer in range(2)
    }

    @pl.when(first)
    def _():
        for layer in range(2):
            for name in "gud":
                loads[name, layer].start()

    def need(*which):
        @pl.when(first)
        def _():
            for one in which:
                loads[one].wait()

    def scale_of(wide):
        return lax.rsqrt(jnp.mean(wide * wide, -1, keepdims=True) + 1e-6)

    x = x_ref[...].astype(F32)
    a0 = (x * scale_of(x)).astype(BF)
    a_buf[...] = a0
    xt_ref[1, 1] = a0.T
    xt_ref[0, 0] = dy_ref[...].T
    need(("g", 0), ("u", 0))

    def panels(body):
        lax.fori_loop(0, PANELS // 3, lambda i, carry: (body(3 * i), body(3 * i + 1), body(3 * i + 2), carry)[3], 0)

    def at(p):
        return pl.ds(pl.multiple_of(p * PANEL, PANEL), PANEL)

    def forward0(p):
        gate, up = dot(a_buf[...], wg[0, :, at(p)]), dot(a_buf[...], wu[0, :, at(p)])
        gate0[:, at(p)], up0[:, at(p)] = gate, up
        ys_ref[1, 0, :, at(p)] = (gate * lax.logistic(gate) * up).astype(BF)

    panels(forward0)
    need(("d", 0))
    h = x + dot(ys_ref[1, 0], wd[0]).astype(BF).astype(F32)
    h = h.astype(BF).astype(F32)
    h_buf[...] = h
    a1 = (h * scale_of(h)).astype(BF)
    a_buf[...] = a1
    xt_ref[0, 1] = a1.T
    need(("g", 1), ("u", 1), ("d", 1))

    def back(d, gate, up):
        d = d.astype(BF).astype(F32)
        s = lax.logistic(gate)
        silu = gate * s
        return (d * up * (s + silu * (1.0 - s))).astype(BF), (d * silu).astype(BF), (silu * up).astype(BF)

    def both1(p):
        gate, up = dot(a_buf[...], wg[1, :, at(p)]), dot(a_buf[...], wu[1, :, at(p)])
        d = dot_t(dy_ref[...], wd[1, at(p), :])
        ys_ref[0, 1, :, at(p)], ys_ref[0, 2, :, at(p)], ys_ref[0, 0, :, at(p)] = back(d, gate, up)

    panels(both1)
    da = dot_t(ys_ref[0, 1], wg[1]).astype(BF).astype(F32) + dot_t(ys_ref[0, 2], wu[1]).astype(BF).astype(F32)
    da = da.astype(BF).astype(F32)
    h = h_buf[...]
    scale = scale_of(h)
    dh = scale * da - h * (scale * scale * scale * jnp.mean(da * h, -1, keepdims=True))
    dh = (dy_ref[...].astype(F32) + dh.astype(BF).astype(F32)).astype(BF)
    a_buf[...] = dh
    xt_ref[1, 0] = dh.T

    def back0(p):
        d = dot_t(a_buf[...], wd[0, at(p), :])
        ys_ref[1, 1, :, at(p)], ys_ref[1, 2, :, at(p)], _ = back(d, gate0[:, at(p)], up0[:, at(p)])

    panels(back0)


def row_wise(x, dy, w_gate, w_up, w_down):
    tokens = x.shape[0]
    return pl.pallas_call(
        rows_kernel,
        grid=(tokens // TB,),
        out_shape=(jax.ShapeDtypeStruct((2, 2, D, tokens), BF), jax.ShapeDtypeStruct((2, 3, tokens, FF), BF)),
        in_specs=[pl.BlockSpec((TB, D), lambda i: (i, 0))] * 2 + [pl.BlockSpec(memory_space=pltpu.HBM)] * 3,
        out_specs=[
            pl.BlockSpec((2, 2, D, TB), lambda i: (0, 0, 0, i)),
            pl.BlockSpec((2, 3, TB, FF), lambda i: (0, 0, i, 0)),
        ],
        scratch_shapes=[
            pltpu.VMEM((2, D, FF), BF),
            pltpu.VMEM((2, D, FF), BF),
            pltpu.VMEM((2, FF, D), BF),
            pltpu.VMEM((TB, FF), F32),
            pltpu.VMEM((TB, FF), F32),
            pltpu.VMEM((TB, D), BF),
            pltpu.VMEM((TB, D), F32),
            pltpu.SemaphoreType.DMA((3, 2)),
        ],
        compiler_params=pltpu.CompilerParams(vmem_limit_bytes=LIMIT, dimension_semantics=("arbitrary",)),
        cost_estimate=pl.CostEstimate(flops=9 * 2 * tokens * D * FF, bytes_accessed=100_000_000, transcendentals=0),
        name="rows",
    )(x, dy, w_gate, w_up, w_down)


def scatter_actions(j, c, at, own, recv, send_sem, recv_sem, finish):
    first, rows = colour(j, c)
    axes = ORDERS[c]

    def add(target, buffers):
        def body(i, carry):
            place = (...,) if i is None else (i,)
            value = target[place].astype(F32)
            for b in buffers:
                value = value + b[place].astype(F32)
            target[place] = value.astype(BF)
            return carry

        if len(target.shape) == 4:
            lax.fori_loop(0, target.shape[0], body, 0)
        else:
            body(None, 0)

    def parts(phase):
        axis = axes[phase]
        h = SIZES[axis] // 2
        fixed = {a: at[a] for a in axes[:phase]}
        buffer = recv[(j * 3 + c) * 3 + phase]
        base = sum(SIZES[a] // 2 for a in axes[:phase])

        def owner(by):
            return dict(fixed, **{axis: shifted(at, axis, by)})

        def slot(s, d):
            index = owner(0)
            if s > 1:
                return (2 * s - 3 + d,)
            place = place_of(index, d, 0, rows)
            return (0,) + tuple(one for a, one in zip(AXES, place[:3], strict=True) if a not in index) + place[3:]

        def copy(g, s, d):
            sign = (1, -1)[d]
            return pltpu.make_async_remote_copy(
                src_ref=own.at[(g, j, *place_of(owner((h - s + 1) * sign), d if s == 1 else None, first, rows))],
                dst_ref=buffer.at[(g, *slot(s, d))],
                send_sem=send_sem.at[g, j, c, d],
                recv_sem=recv_sem.at[g, j, c, base + s - 1, d],
                device_id=device(at, axis, shifted(at, axis, sign)),
                device_id_type=MESH,
            )

        def step(g, s):
            for d in range(2):
                copy(g, s, d).wait_recv()
            if s < h:
                for d in range(2):
                    by = (h - s) * (1, -1)[d]
                    place = place_of(owner(by), d if s == 1 else None, first, rows)
                    add(own.at[(g, j, *place)], [buffer.at[(g, *slot(s, d))]])
            else:
                place = place_of(owner(0), None, first, rows)
                add(own.at[(g, j, *place)], [buffer.at[(g, *slot(s, d))] for d in range(2)])

        return h, copy, step

    def action(number):
        def run(g):
            left, phase = number, 0
            while phase < 3 and left > SIZES[axes[phase]] // 2:
                left -= SIZES[axes[phase]] // 2
                phase += 1
            h, copy, step = parts(phase)
            if left > 0:
                step(g, left)
            before = [copy(g, left, d) for d in range(2)] if left > 0 else []
            if left == h:
                if phase == 2:
                    for one in before:
                        one.wait_send()
                    finish(g, j, c, own.at[(g, j, *place_of(at, None, first, rows))])
                    return
                _, copy, _ = parts(phase + 1)
                left = 0
            for one in before:
                one.wait_send()
            for d in range(2):
                copy(g, left + 1, d).start()

        return run

    return [action(n) for n in range(1 + sum(SIZES[a] // 2 for a in axes))]


def scatter_order(panel_time=1.15, period=42.0):
    streams = {(j, c): scatter_steps(j, c) for j in range(3) for c in range(3)}
    events = serve_order(streams, {(j, c): PANELS * (j + 1) for j, c in streams}, 3 * PANELS, panel_time)
    panel_ends = [t for t, key in events if not isinstance(key, tuple)]
    slots = [[] for _ in range(len(panel_ends) + 1)]
    count = {key: 0 for key in streams}
    placed = []
    for t, key in events:
        if isinstance(key, tuple):
            placed.append((t % period, int(t // period), key, count[key]))
            count[key] += 1
    for t, late, key, number in sorted(placed):
        slot = sum(end <= t for end in panel_ends) - 1
        slots[max(slot, 0) if slot < len(panel_ends) - 1 or t < panel_ends[-1] + 0.5 else len(panel_ends)].append((late, key, number))
    return slots


def scatter_kernel(xt_ref, ys_ref, shard_ref, squares_ref, own, *refs):
    recv, refs = refs[:27], refs[27:]
    xbuf, ybuf, x_sem, y_sem, send_sem, recv_sem = refs
    at = here()
    total = 3 * PANELS

    def load_x(g, kind):
        return pltpu.make_async_copy(xt_ref.at[g, kind], xbuf.at[kind], x_sem.at[kind])

    def load_y(g, n):
        lanes = pl.ds(pl.multiple_of((n % PANELS) * PANEL, PANEL), PANEL)
        return pltpu.make_async_copy(ys_ref.at[g, n // PANELS, :, lanes], ybuf.at[n % 3], y_sem.at[n % 3])

    load_x(0, 0).start()
    load_y(0, 0).start()
    load_y(0, 1).start()
    load_x(0, 1).start()
    squares_ref[...] = jnp.zeros_like(squares_ref)
    for g in range(2):
        for j in range(3):
            for z in (6, 7):
                own[g, j, 3, 3, z] = jnp.zeros((SHARD, LANES), BF)
    meet(at)

    def finish(g, j, c, region):
        first, rows = colour(j, c)
        value = region[...]
        shard_ref[j, g, pl.ds(first, rows), :] = value
        wide = value.astype(F32)
        squares_ref[...] += jnp.sum((wide * wide).reshape(rows // 8, 8, LANES), axis=0)

    actions = {(j, c): scatter_actions(j, c, at, own, recv, send_sem, recv_sem, finish) for j in range(3) for c in range(3)}
    slots = scatter_order()

    def group(i, carry):
        def slot(n, carry):
            @pl.when(jnp.logical_and(n < total, i < 2))
            def _():
                j, p = n // PANELS, n % PANELS
                kind = jnp.minimum(j, 1)

                @pl.when(n == 0)
                def _():
                    load_x(i, 0).wait()

                @pl.when(n == PANELS)
                def _():
                    load_x(i, 1).wait()

                    @pl.when(i < 1)
                    def _():
                        load_x(i + 1, 0).start()

                load_y(i, n).wait()

                @pl.when(n + 2 < total)
                def _():
                    load_y(i, n + 2).start()

                @pl.when(jnp.logical_and(n + 2 >= total, i < 1))
                def _():
                    load_y(i + 1, n + 2 - total).start()

                out = dot(xbuf[kind], ybuf[n % 3])
                for half in range(PANEL // LANES):
                    for b in range(D // SHARD):
                        d = (2 * p + half) * (D // SHARD) + b
                        block = out[b * SHARD : (b + 1) * SHARD, half * LANES : (half + 1) * LANES]
                        own[i, j, d // 32, (d // 8) % 4, d % 8] = block.astype(BF)

                @pl.when(jnp.logical_and(n == total - 1, i < 1))
                def _():
                    load_x(i + 1, 1).start()

            for number, todo in enumerate(slots):
                if todo:

                    @pl.when(n == number)
                    def _():
                        for late, key, which in todo:

                            @pl.when(i > 0 if late else i < 2)
                            def _():
                                actions[key][which](i - 1 if late else i)

            return carry

        lax.fori_loop(0, total + 1, slot, 0)
        return carry

    lax.fori_loop(0, 3, group, 0)


def recv_shapes():
    shapes = []
    for j in range(3):
        for c in range(3):
            for phase in range(3):
                axes = ORDERS[c]
                left = tuple(SIZES[a] for a in AXES if a not in axes[: phase + 1])
                shapes.append(pltpu.VMEM((2, SIZES[axes[phase]] - 1, *left, ROWS[j][c], LANES), BF))
    return shapes


def scattered(xt, ys):
    sent = 6 * D * FF * 2
    return pl.pallas_call(
        scatter_kernel,
        out_shape=(jax.ShapeDtypeStruct((3, 2, SHARD, LANES), BF), jax.ShapeDtypeStruct((8, LANES), F32)),
        in_specs=[pl.BlockSpec(memory_space=pltpu.HBM)] * 2,
        out_specs=[pl.BlockSpec(memory_space=pltpu.VMEM)] * 2,
        scratch_shapes=[
            pltpu.VMEM((2, 3, 4, 4, 8, SHARD, LANES), BF),
            *recv_shapes(),
            pltpu.VMEM((2, D, TOKENS), BF),
            pltpu.VMEM((3, TOKENS, PANEL), BF),
            pltpu.SemaphoreType.DMA((2,)),
            pltpu.SemaphoreType.DMA((3,)),
            pltpu.SemaphoreType.DMA((2, 3, 3, 2)),
            pltpu.SemaphoreType.DMA((2, 3, 3, 8, 2)),
        ],
        compiler_params=pltpu.CompilerParams(collective_id=0, has_side_effects=True, vmem_limit_bytes=LIMIT),
        cost_estimate=pl.CostEstimate(flops=6 * 2 * TOKENS * D * FF, bytes_accessed=3 * sent, transcendentals=0),
        name="scatter",
    )(xt, ys)


def gather_actions(j, c, at, full, send_sem, recv_sem):
    first, rows = colour(j, c)
    axes = ORDERS[c]
    names = []
    for phase in (2, 1, 0):
        for s in range(1, SIZES[axes[phase]] // 2 + 1):
            names.append((phase, s))

    def copy(number, d):
        phase, s = names[number]
        axis = axes[phase]
        h = SIZES[axis] // 2
        sign = (1, -1)[d]
        index = {a: at[a] for a in axes[:phase]}
        index[axis] = shifted(at, axis, -(s - 1) * sign)
        place = (j, slice(None), *place_of(index, d if s == h else None, first, rows))
        return pltpu.make_async_remote_copy(
            src_ref=full.at[place],
            dst_ref=full.at[place],
            send_sem=send_sem.at[j, c, d],
            recv_sem=recv_sem.at[j, c, number, d],
            device_id=device(at, axis, shifted(at, axis, sign)),
            device_id_type=MESH,
        )

    def arriving(number, d):
        phase, s = names[number]
        axis = axes[phase]
        h = SIZES[axis] // 2
        sign = (1, -1)[d]
        index = {a: at[a] for a in axes[:phase]}
        index[axis] = shifted(at, axis, -s * sign)
        place = (j, slice(None), *place_of(index, d if s == h else None, first, rows))
        return pltpu.make_async_remote_copy(
            src_ref=full.at[place],
            dst_ref=full.at[place],
            send_sem=send_sem.at[j, c, d],
            recv_sem=recv_sem.at[j, c, number, d],
            device_id=device(at, axis, shifted(at, axis, sign)),
            device_id_type=MESH,
        )

    def action(number):
        def run():
            if number > 0:
                for d in range(2):
                    arriving(number - 1, d).wait_recv()
                for d in range(2):
                    copy(number - 1, d).wait_send()
            if number < len(names):
                for d in range(2):
                    copy(number, d).start()

        return run

    return [action(n) for n in range(len(names) + 1)]


def sum_actions(at, squares_ref, total_ref, boxes, send_sem, recv_sem):
    order = ("z", "x", "y")

    def copies(n):
        axis = order[n]
        base = sum(SIZES[a] - 1 for a in order[:n])
        box = boxes[axis]
        return [
            pltpu.make_async_remote_copy(
                src_ref=box.at[at[axis]],
                dst_ref=box.at[at[axis]],
                send_sem=send_sem.at[base + by - 1],
                recv_sem=recv_sem.at[base + by - 1],
                device_id=device(at, axis, shifted(at, axis, by)),
                device_id_type=MESH,
            )
            for by in range(1, SIZES[axis])
        ]

    def action(n):
        def run():
            if n == 0:
                value = squares_ref[...]
            else:
                for one in copies(n - 1):
                    one.wait()
                box = boxes[order[n - 1]]
                value = box[0]
                for i in range(1, SIZES[order[n - 1]]):
                    value = value + box[i]
            if n == len(order):
                total_ref[...] = value
                return
            boxes[order[n]][at[order[n]]] = value
            for one in copies(n):
                one.start()

        return run

    return [action(n) for n in range(len(order) + 1)]


def gather_kernel(shard_ref, squares_ref, out_ref, total_ref, full, box_x, box_y, box_z, load_sem, out_sem, send_sem, recv_sem, sum_send, sum_recv):
    at = here()
    mine = full.at[:, :, at["x"], at["y"], at["z"]]
    load = pltpu.make_async_copy(shard_ref, mine, load_sem)
    load.start()
    meet(at)
    load.wait()
    sums = sum_actions(at, squares_ref, total_ref, {"x": box_x, "y": box_y, "z": box_z}, sum_send, sum_recv)
    sums[0]()
    streams = {(j, c): gather_steps(j, c) for j in range(3) for c in range(3)}
    events = serve_order(streams, dict.fromkeys(streams, 0), 0, 0.0)
    actions = {(j, c): gather_actions(j, c, at, full, send_sem, recv_sem) for j, c in streams}
    count = dict.fromkeys(streams, 0)
    left = {j: 3 for j in range(3)}
    outs = [pltpu.make_async_copy(full.at[j], out_ref.at[j], out_sem.at[j]) for j in range(3)]
    summed = 1
    for t, key in events:
        while summed < len(sums) and t > 5.0 * summed:
            sums[summed]()
            summed += 1
        actions[key][count[key]]()
        count[key] += 1
        if count[key] == len(actions[key]):
            left[key[0]] -= 1
            if left[key[0]] == 0:
                outs[key[0]].start()
    for one in outs:
        one.wait()


def gathered(shards, squares):
    sent = 6 * D * FF * 2
    return pl.pallas_call(
        gather_kernel,
        out_shape=(jax.ShapeDtypeStruct((3, 2, 4, 4, 8, SHARD, LANES), BF), jax.ShapeDtypeStruct((8, LANES), F32)),
        in_specs=[pl.BlockSpec(memory_space=pltpu.HBM), pl.BlockSpec(memory_space=pltpu.VMEM)],
        out_specs=[pl.BlockSpec(memory_space=pltpu.HBM), pl.BlockSpec(memory_space=pltpu.VMEM)],
        scratch_shapes=[
            pltpu.VMEM((3, 2, 4, 4, 8, SHARD, LANES), BF),
            pltpu.VMEM((4, 8, LANES), F32),
            pltpu.VMEM((4, 8, LANES), F32),
            pltpu.VMEM((8, 8, LANES), F32),
            pltpu.SemaphoreType.DMA,
            pltpu.SemaphoreType.DMA((3,)),
            pltpu.SemaphoreType.DMA((3, 3, 2)),
            pltpu.SemaphoreType.DMA((3, 3, 8, 2)),
            pltpu.SemaphoreType.DMA((13,)),
            pltpu.SemaphoreType.DMA((13,)),
        ],
        compiler_params=pltpu.CompilerParams(collective_id=1, has_side_effects=True, vmem_limit_bytes=LIMIT),
        cost_estimate=pl.CostEstimate(flops=sent * 100, bytes_accessed=2 * sent, transcendentals=0),
        name="gather",
    )(shards, squares)


def adamw_kernel(total_ref, g_ref, *refs):
    ins, outs, factor_ref = refs[:9], refs[9:18], refs[18]

    @pl.when(jnp.logical_and(pl.program_id(0) == 0, pl.program_id(1) == 0))
    def _():
        mean = jnp.sum(total_ref[...], keepdims=True) * (1.0 / (6 * D * FF))
        factor_ref[...] = jnp.broadcast_to(jnp.minimum(1.0, 0.5 * lax.rsqrt(mean + 1e-30)), factor_ref.shape)

    factor = factor_ref[0:1, :]

    def one(j, g, place):
        w_ref, m_ref, v_ref = ins[3 * j : 3 * j + 3]
        wo_ref, mo_ref, vo_ref = outs[3 * j : 3 * j + 3]
        w = w_ref[place].astype(F32)
        m = 0.9 * m_ref[place] + 0.1 * g
        v = 0.95 * v_ref[place] + 0.05 * g * g
        step = m * lax.rsqrt(v + 1e-8) + 0.1 * w
        wo_ref[place] = (w - 0.02 * step).astype(BF)
        mo_ref[place] = m
        vo_ref[place] = v

    for half in range(PANEL // LANES):
        lanes = pl.ds(half * LANES, LANES)

        def body(i, carry):
            here_rows = pl.ds(pl.multiple_of(half * D + i * 128, 128), 128)
            rows = pl.ds(pl.multiple_of(i * 128, 128), 128)
            for j in (1, 2):
                one(j, g_ref[j, here_rows, :].astype(F32) * factor, (rows, lanes))
            return carry

        lax.fori_loop(0, D // 128, body, 0)
        for i in range(D // 128):
            g = g_ref[0, pl.ds(half * D + i * 128, 128), :].astype(F32) * factor
            one(0, g.T, (lanes, pl.ds(i * 128, 128)))


def adamw(total, g, weights):
    wide = pl.BlockSpec((None, D, PANEL), lambda l, p: (l, 0, p))
    tall = pl.BlockSpec((None, PANEL, D), lambda l, p: (l, p, 0))
    specs = [tall] * 3 + [wide] * 6
    arrays = [a for one in weights for a in one]
    return pl.pallas_call(
        adamw_kernel,
        grid=(2, PANELS),
        out_shape=[jax.ShapeDtypeStruct(a.shape, a.dtype) for a in arrays],
        in_specs=[
            pl.BlockSpec((8, LANES), lambda l, p: (0, 0)),
            pl.BlockSpec((3, None, PANEL // LANES * D, LANES), lambda l, p: (0, 1 - l, p, 0)),
            *specs,
        ],
        out_specs=specs,
        scratch_shapes=[pltpu.VMEM((8, LANES), F32)],
        compiler_params=pltpu.CompilerParams(vmem_limit_bytes=LIMIT, dimension_semantics=("arbitrary", "arbitrary")),
        cost_estimate=pl.CostEstimate(flops=6 * D * FF * 30, bytes_accessed=6 * D * FF * 22, transcendentals=6 * D * FF),
        name="adamw",
    )(total, g, *arrays)


def solution(mesh):
    def step(x, dy, w_gate, w_up, w_down, m_gate, m_up, m_down, v_gate, v_up, v_down):
        xt, ys = row_wise(x[0], dy[0], w_gate, w_up, w_down)
        shards, squares = scattered(xt, ys)
        full, total = gathered(shards, squares)
        new = adamw(
            total,
            full.reshape(3, 2, 128 * SHARD, LANES),
            ((w_down, m_down, v_down), (w_gate, m_gate, v_gate), (w_up, m_up, v_up)),
        )
        return tuple(new[3 * j + which] for which in range(3) for j in (1, 2, 0))

    return jax.shard_map(
        step,
        mesh=mesh,
        in_specs=(P(("rep", "dp"), None, None),) * 2 + (P(None, None, None),) * 9,
        out_specs=(P("rep", None, None),) * 9,
        check_vma=False,
    )
```

```python
import functools

import jax
import jax.numpy as jnp
from jax import lax
from jax.experimental import pallas as pl
from jax.experimental.pallas import tpu as pltpu
from jax.sharding import PartitionSpec as P

BF, F32 = jnp.bfloat16, jnp.float32
MESH = pl.DeviceIdType.MESH
SIZES = {"x": 4, "y": 4, "z": 8}
AXES = ("x", "y", "z")
LANES = 128
SHARD = 128
D, FF, TOKENS = 896, 2304, 2048
PANEL = 256
PANELS = FF // PANEL
LIMIT = 66_900_000
ORDERS = tuple((("z", *second), ("x", "y", "z"), ("y", "x", "z")) for second in (("x", "y"), ("y", "x"), ("x", "y")))
ROWS = ((48, 48, 32), (48, 32, 48), (32, 48, 48))


def colour(j, c):
    return sum(ROWS[j][:c]), ROWS[j][c]


def here():
    d = lax.axis_index("dp")
    return {"x": d // 32, "y": (d // 8) % 4, "z": d % 8}


def device(at, axis, value):
    at = dict(at, **{axis: value})
    return {"dp": (at["x"] * 4 + at["y"]) * 8 + at["z"]}


def shifted(at, axis, by):
    n = SIZES[axis]
    return (at[axis] + (by % n)) % n


def meet(at):
    barrier = pltpu.get_barrier_semaphore()
    peers = [(axis, by) for axis in AXES for by in range(1, SIZES[axis])]
    for axis, by in peers:
        pl.semaphore_signal(barrier, inc=1, device_id=device(at, axis, shifted(at, axis, by)), device_id_type=MESH)
    pl.semaphore_wait(barrier, len(peers))


def place_of(fixed, half, first, rows):
    place, halved = [], half is None
    for a in AXES:
        if a in fixed:
            place.append(fixed[a])
        elif not halved:
            n = SIZES[a] // 2
            place.append(pl.ds(half * n, n))
            halved = True
        else:
            place.append(slice(None))
    begin, size = first, rows
    if not halved:
        one = (rows // 2 + 15) // 16 * 16
        begin, size = (first, one) if half == 0 else (first + one, rows - one)
    return tuple(place) + (pl.ds(begin, size), slice(None))


RATE, LATENCY, SERVE = 45.0e3, 2.2, 0.3


def bytes_of(j, c, phase, part):
    size = SHARD * SHARD * LANES * 2 * ROWS[j][c] // SHARD
    for axis in ORDERS[j][c][: phase + 1]:
        size //= SIZES[axis]
    return size * part


def gather_steps(j, c):
    out = []
    for phase, axis in reversed(list(enumerate(ORDERS[j][c]))):
        h = SIZES[axis] // 2
        for s in range(1, h + 1):
            out.append((axis, 2 * bytes_of(j, c, phase, 0.5 if s == h else 1)))
    return out


def gather_order(streams):
    free = dict.fromkeys(AXES, 0.0)
    arrival, position = {}, {}
    now, out = 0.0, []
    waiting = list(streams)

    def send(key, at):
        axis, size = streams[key][at]
        free[axis] = max(now, free[axis]) + size / RATE
        arrival[key], position[key] = free[axis] + LATENCY, at

    while waiting or arrival:
        choices = sorted((t, key) for key, t in arrival.items())
        start = next((key for key in waiting if free[streams[key][0][0]] < now + 3.0), None)
        if start is not None:
            now += SERVE
            out.append((now, start))
            waiting.remove(start)
            send(start, 0)
        elif choices and choices[0][0] <= now:
            key = choices[0][1]
            now += SERVE
            out.append((now, key))
            del arrival[key]
            if position[key] + 1 < len(streams[key]):
                send(key, position[key] + 1)
        else:
            later = [choices[0][0]] if choices else []
            later += [free[streams[key][0][0]] - 3.0 for key in waiting]
            now = max(now + 0.01, min(later))
    return out


TB = 512


def dot(a, b):
    return lax.dot_general(a, b, (((1,), (0,)), ((), ())), preferred_element_type=F32)


def dot_t(a, b):
    return lax.dot_general(a, b, (((1,), (1,)), ((), ())), preferred_element_type=F32)


def rows_kernel(x_ref, dy_ref, wg_ref, wu_ref, wd_ref, xt_hbm, ys_hbm, wg, wu, wd, gate0, up0, a_buf, h_buf, xt_ref, ys_ref, load_sem, xt_sem, ys_sem):
    block = pl.program_id(0)
    first, last = block == 0, block == pl.num_programs(0) - 1
    loads = {
        (name, layer): pltpu.make_async_copy(ref.at[layer], buf.at[layer], load_sem.at[n, layer])
        for n, (name, ref, buf) in enumerate((("g", wg_ref, wg), ("u", wu_ref, wu), ("d", wd_ref, wd)))
        for layer in range(2)
    }

    @pl.when(first)
    def _():
        for layer in range(2):
            for name in "gud":
                loads[name, layer].start()

    def need(*which):
        @pl.when(first)
        def _():
            for one in which:
                loads[one].wait()

    tokens = pl.ds(pl.multiple_of(block * TB, TB), TB)

    def xt_out(*at):
        return pltpu.make_async_copy(xt_ref.at[at], xt_hbm.at[(*at, slice(None), tokens)], xt_sem.at[at])

    def ys_out(*at):
        return pltpu.make_async_copy(ys_ref.at[at], ys_hbm.at[(*at, tokens, slice(None))], ys_sem.at[at])

    def free(*outs):
        @pl.when(jnp.logical_not(first))
        def _():
            for one in outs:
                one.wait()

    def scale_of(wide):
        return lax.rsqrt(jnp.mean(wide * wide, -1, keepdims=True) + 1e-6)

    x = x_ref[...].astype(F32)
    a0 = (x * scale_of(x)).astype(BF)
    a_buf[...] = a0
    free(xt_out(1, 1), xt_out(0, 0))
    xt_ref[1, 1] = a0.T
    xt_ref[0, 0] = dy_ref[...].T
    xt_out(1, 1).start()
    xt_out(0, 0).start()
    free(ys_out(1, 0))
    need(("g", 0), ("u", 0))

    def panels(body):
        lax.fori_loop(0, PANELS // 3, lambda i, carry: (body(3 * i), body(3 * i + 1), body(3 * i + 2), carry)[3], 0)

    def at(p):
        return pl.ds(pl.multiple_of(p * PANEL, PANEL), PANEL)

    def forward0(p):
        gate, up = dot(a_buf[...], wg[0, :, at(p)]), dot(a_buf[...], wu[0, :, at(p)])
        gate0[:, at(p)], up0[:, at(p)] = gate, up
        ys_ref[1, 0, :, at(p)] = (gate * lax.logistic(gate) * up).astype(BF)

    panels(forward0)
    ys_out(1, 0).start()
    need(("d", 0))
    h = x + dot(ys_ref[1, 0], wd[0]).astype(BF).astype(F32)
    h = h.astype(BF).astype(F32)
    h_buf[...] = h
    a1 = (h * scale_of(h)).astype(BF)
    a_buf[...] = a1
    free(xt_out(0, 1))
    xt_ref[0, 1] = a1.T
    xt_out(0, 1).start()
    free(ys_out(0, 0), ys_out(0, 1), ys_out(0, 2))
    need(("g", 1), ("u", 1), ("d", 1))

    def back(d, gate, up):
        d = d.astype(BF).astype(F32)
        s = lax.logistic(gate)
        silu = gate * s
        return (d * up * (s + silu * (1.0 - s))).astype(BF), (d * silu).astype(BF), (silu * up).astype(BF)

    def both1(p):
        gate, up = dot(a_buf[...], wg[1, :, at(p)]), dot(a_buf[...], wu[1, :, at(p)])
        d = dot_t(dy_ref[...], wd[1, at(p), :])
        ys_ref[0, 1, :, at(p)], ys_ref[0, 2, :, at(p)], ys_ref[0, 0, :, at(p)] = back(d, gate, up)

    panels(both1)
    for j in range(3):
        ys_out(0, j).start()
    da = dot_t(ys_ref[0, 1], wg[1]).astype(BF).astype(F32) + dot_t(ys_ref[0, 2], wu[1]).astype(BF).astype(F32)
    da = da.astype(BF).astype(F32)
    h = h_buf[...]
    scale = scale_of(h)
    dh = scale * da - h * (scale * scale * scale * jnp.mean(da * h, -1, keepdims=True))
    dh = (dy_ref[...].astype(F32) + dh.astype(BF).astype(F32)).astype(BF)
    a_buf[...] = dh
    free(xt_out(1, 0))
    xt_ref[1, 0] = dh.T
    xt_out(1, 0).start()
    free(ys_out(1, 1), ys_out(1, 2))

    def back0(p):
        d = dot_t(a_buf[...], wd[0, at(p), :])
        ys_ref[1, 1, :, at(p)], ys_ref[1, 2, :, at(p)], _ = back(d, gate0[:, at(p)], up0[:, at(p)])

    panels(back0)
    for j in (1, 2):
        ys_out(1, j).start()

    @pl.when(last)
    def _():
        for g in range(2):
            for kind in range(2):
                xt_out(g, kind).wait()
            for j in range(3):
                ys_out(g, j).wait()


def row_wise(x, dy, w_gate, w_up, w_down):
    tokens = x.shape[0]
    return pl.pallas_call(
        rows_kernel,
        grid=(tokens // TB,),
        out_shape=(jax.ShapeDtypeStruct((2, 2, D, tokens), BF), jax.ShapeDtypeStruct((2, 3, tokens, FF), BF)),
        in_specs=[pl.BlockSpec((TB, D), lambda i: (i, 0))] * 2 + [pl.BlockSpec(memory_space=pltpu.HBM)] * 3,
        out_specs=[pl.BlockSpec(memory_space=pltpu.HBM)] * 2,
        scratch_shapes=[
            pltpu.VMEM((2, D, FF), BF),
            pltpu.VMEM((2, D, FF), BF),
            pltpu.VMEM((2, FF, D), BF),
            pltpu.VMEM((TB, FF), F32),
            pltpu.VMEM((TB, FF), F32),
            pltpu.VMEM((TB, D), BF),
            pltpu.VMEM((TB, D), F32),
            pltpu.VMEM((2, 2, D, TB), BF),
            pltpu.VMEM((2, 3, TB, FF), BF),
            pltpu.SemaphoreType.DMA((3, 2)),
            pltpu.SemaphoreType.DMA((2, 2)),
            pltpu.SemaphoreType.DMA((2, 3)),
        ],
        compiler_params=pltpu.CompilerParams(vmem_limit_bytes=LIMIT, dimension_semantics=("arbitrary",)),
        cost_estimate=pl.CostEstimate(flops=9 * 2 * tokens * D * FF, bytes_accessed=100_000_000, transcendentals=0),
        name="rows",
    )(x, dy, w_gate, w_up, w_down)


def scatter_actions(j, c, at, own, recv, send_sem, recv_sem, finish):
    first, rows = colour(j, c)
    axes = ORDERS[j][c]

    def add(target, buffers):
        def body(i, carry):
            place = (...,) if i is None else (i,)
            value = target[place].astype(F32)
            for b in buffers:
                value = value + b[place].astype(F32)
            target[place] = value.astype(BF)
            return carry

        if len(target.shape) == 4:
            lax.fori_loop(0, target.shape[0], body, 0)
        else:
            body(None, 0)

    def parts(phase):
        axis = axes[phase]
        h = SIZES[axis] // 2
        fixed = {a: at[a] for a in axes[:phase]}
        buffer = recv[(j * 3 + c) * 3 + phase]
        base = sum(SIZES[a] // 2 for a in axes[:phase])

        def owner(by):
            return dict(fixed, **{axis: shifted(at, axis, by)})

        def slot(s, d):
            index = owner(0)
            if s > 1:
                return (2 * s - 3 + d,)
            place = place_of(index, d, 0, rows)
            return (0,) + tuple(one for a, one in zip(AXES, place[:3], strict=True) if a not in index) + place[3:]

        def copy(g, s, d):
            sign = (1, -1)[d]
            return pltpu.make_async_remote_copy(
                src_ref=own.at[(g, j, *place_of(owner((h - s + 1) * sign), d if s == 1 else None, first, rows))],
                dst_ref=buffer.at[(g, *slot(s, d))],
                send_sem=send_sem.at[g, j, c, d],
                recv_sem=recv_sem.at[g, j, c, base + s - 1, d],
                device_id=device(at, axis, shifted(at, axis, sign)),
                device_id_type=MESH,
            )

        def step(g, s):
            for d in range(2):
                copy(g, s, d).wait_recv()
            if s < h:
                for d in range(2):
                    by = (h - s) * (1, -1)[d]
                    place = place_of(owner(by), d if s == 1 else None, first, rows)
                    add(own.at[(g, j, *place)], [buffer.at[(g, *slot(s, d))]])
            else:
                place = place_of(owner(0), None, first, rows)
                add(own.at[(g, j, *place)], [buffer.at[(g, *slot(s, d))] for d in range(2)])

        return h, copy, step

    def action(number):
        def run(g):
            left, phase = number, 0
            while phase < 3 and left > SIZES[axes[phase]] // 2:
                left -= SIZES[axes[phase]] // 2
                phase += 1
            h, copy, step = parts(phase)
            if left > 0:
                step(g, left)
            before = [copy(g, left, d) for d in range(2)] if left > 0 else []
            if left == h:
                if phase == 2:
                    for one in before:
                        one.wait_send()
                    finish(g, j, c, own.at[(g, j, *place_of(at, None, first, rows))])
                    return
                _, copy, _ = parts(phase + 1)
                left = 0
            for one in before:
                one.wait_send()
            for d in range(2):
                copy(g, left + 1, d).start()

        return run

    return [action(n) for n in range(1 + sum(SIZES[a] // 2 for a in axes))]


SLOTS = (
    ((2, 8, 5),),
    ((2, 1, 6),),
    ((1, 7, 1),),
    (),
    ((1, 8, 1), (1, 6, 2),),
    ((2, 2, 6), (1, 3, 2),),
    ((2, 6, 6),),
    ((2, 0, 6), (1, 4, 2), (2, 5, 6), (2, 4, 6), (2, 7, 6),),
    ((0, 1, 0), (0, 0, 0), (0, 2, 0), (1, 5, 2),),
    ((1, 2, 3),),
    ((1, 6, 3),),
    ((1, 0, 4), (2, 8, 6), (2, 3, 6),),
    (),
    ((1, 7, 2), (0, 0, 1), (1, 1, 3), (1, 3, 3), (1, 8, 2),),
    ((2, 1, 7), (0, 1, 1),),
    ((0, 2, 1),),
    ((2, 5, 7),),
    ((0, 5, 0),),
    ((1, 4, 3), (1, 5, 3),),
    ((2, 4, 7),),
    ((0, 3, 0),),
    ((1, 6, 4), (0, 0, 2), (0, 4, 0),),
    ((2, 2, 7), (1, 7, 3),),
    (),
    ((1, 8, 3),),
    (),
    ((2, 0, 7), (2, 6, 7), (2, 7, 7), (0, 8, 0), (0, 6, 0), (2, 8, 7), (1, 2, 4), (1, 6, 5), (0, 7, 0), (1, 4, 4), (1, 1, 4), (0, 1, 2), (0, 3, 1), (1, 5, 4), (1, 3, 4), (2, 3, 7), (1, 0, 5), (0, 5, 1), (2, 1, 8), (2, 5, 8), (1, 7, 4), (0, 2, 2), (1, 8, 4), (0, 6, 1), (2, 4, 8), (1, 1, 5), (1, 2, 5), (2, 0, 8), (2, 2, 8), (0, 4, 1), (2, 6, 8), (1, 5, 5), (2, 7, 8), (0, 0, 3), (1, 4, 5), (1, 3, 5), (2, 8, 8), (1, 7, 5), (2, 3, 8),),
    (),
)


def scatter_kernel(xt_ref, ys_ref, shard_ref, squares_ref, own, *refs):
    recv, refs = refs[:27], refs[27:]
    xbuf, ybuf, x_sem, y_sem, send_sem, recv_sem = refs
    at = here()
    total = 3 * PANELS

    def load_x(g, kind):
        return pltpu.make_async_copy(xt_ref.at[g, kind], xbuf.at[kind], x_sem.at[kind])

    def load_y(g, n):
        lanes = pl.ds(pl.multiple_of((n % PANELS) * PANEL, PANEL), PANEL)
        return pltpu.make_async_copy(ys_ref.at[g, n // PANELS, :, lanes], ybuf.at[n % 3], y_sem.at[n % 3])

    load_x(0, 0).start()
    load_y(0, 0).start()
    load_y(0, 1).start()
    load_x(0, 1).start()
    squares_ref[...] = jnp.zeros_like(squares_ref)
    for g in range(2):
        for j in range(3):
            for z in (6, 7):
                own[g, j, 3, 3, z] = jnp.zeros((SHARD, LANES), BF)
    meet(at)

    def finish(g, j, c, region):
        first, rows = colour(j, c)
        value = region[...]
        shard_ref[j, g, pl.ds(first, rows), :] = value
        wide = value.astype(F32)
        squares_ref[...] += jnp.sum((wide * wide).reshape(rows // 8, 8, LANES), axis=0)

    actions = [scatter_actions(j, c, at, own, recv, send_sem, recv_sem, finish) for j in range(3) for c in range(3)]
    rounds = 2 + max(late for todo in SLOTS for late, _, _ in todo)

    def group(i, carry):
        def slot(n, carry):
            @pl.when(jnp.logical_and(n < total, i < 2))
            def _():
                j, p = n // PANELS, n % PANELS
                kind = jnp.minimum(j, 1)

                @pl.when(n == 0)
                def _():
                    load_x(i, 0).wait()

                @pl.when(n == PANELS)
                def _():
                    load_x(i, 1).wait()

                    @pl.when(i < 1)
                    def _():
                        load_x(i + 1, 0).start()

                load_y(i, n).wait()

                @pl.when(n + 2 < total)
                def _():
                    load_y(i, n + 2).start()

                @pl.when(jnp.logical_and(n + 2 >= total, i < 1))
                def _():
                    load_y(i + 1, n + 2 - total).start()

                out = dot(xbuf[kind], ybuf[n % 3])
                for half in range(PANEL // LANES):
                    for b in range(D // SHARD):
                        d = (2 * p + half) * (D // SHARD) + b
                        block = out[b * SHARD : (b + 1) * SHARD, half * LANES : (half + 1) * LANES]
                        own[i, j, d // 32, (d // 8) % 4, d % 8] = block.astype(BF)

                @pl.when(jnp.logical_and(n == total - 1, i < 1))
                def _():
                    load_x(i + 1, 1).start()

            def serve(todo):
                for late, key, which in todo:
                    pl.when(jnp.logical_and(i >= late, i < 2 + late))(functools.partial(actions[key][which], i - late))

            for number, todo in enumerate(SLOTS):
                if todo:
                    pl.when(n == number)(functools.partial(serve, todo))
            return carry

        lax.fori_loop(0, total + 1, slot, 0)
        return carry

    lax.fori_loop(0, rounds, group, 0)


def recv_shapes():
    shapes = []
    for j in range(3):
        for c in range(3):
            for phase in range(3):
                axes = ORDERS[j][c]
                left = tuple(SIZES[a] for a in AXES if a not in axes[: phase + 1])
                shapes.append(pltpu.VMEM((2, SIZES[axes[phase]] - 1, *left, ROWS[j][c], LANES), BF))
    return shapes


def scattered(xt, ys):
    sent = 6 * D * FF * 2
    return pl.pallas_call(
        scatter_kernel,
        out_shape=(jax.ShapeDtypeStruct((3, 2, SHARD, LANES), BF), jax.ShapeDtypeStruct((8, LANES), F32)),
        in_specs=[pl.BlockSpec(memory_space=pltpu.HBM)] * 2,
        out_specs=[pl.BlockSpec(memory_space=pltpu.VMEM)] * 2,
        scratch_shapes=[
            pltpu.VMEM((2, 3, 4, 4, 8, SHARD, LANES), BF),
            *recv_shapes(),
            pltpu.VMEM((2, D, TOKENS), BF),
            pltpu.VMEM((3, TOKENS, PANEL), BF),
            pltpu.SemaphoreType.DMA((2,)),
            pltpu.SemaphoreType.DMA((3,)),
            pltpu.SemaphoreType.DMA((2, 3, 3, 2)),
            pltpu.SemaphoreType.DMA((2, 3, 3, 8, 2)),
        ],
        compiler_params=pltpu.CompilerParams(collective_id=0, has_side_effects=True, vmem_limit_bytes=LIMIT),
        cost_estimate=pl.CostEstimate(flops=6 * 2 * TOKENS * D * FF, bytes_accessed=3 * sent, transcendentals=0),
        name="scatter",
    )(xt, ys)


def gather_actions(j, c, at, full, send_sem, recv_sem):
    first, rows = colour(j, c)
    axes = ORDERS[j][c]
    names = []
    for phase in (2, 1, 0):
        for s in range(1, SIZES[axes[phase]] // 2 + 1):
            names.append((phase, s))

    def copy(number, d):
        phase, s = names[number]
        axis = axes[phase]
        h = SIZES[axis] // 2
        sign = (1, -1)[d]
        index = {a: at[a] for a in axes[:phase]}
        index[axis] = shifted(at, axis, -(s - 1) * sign)
        place = (j, slice(None), *place_of(index, d if s == h else None, first, rows))
        return pltpu.make_async_remote_copy(
            src_ref=full.at[place],
            dst_ref=full.at[place],
            send_sem=send_sem.at[j, c, d],
            recv_sem=recv_sem.at[j, c, number, d],
            device_id=device(at, axis, shifted(at, axis, sign)),
            device_id_type=MESH,
        )

    def arriving(number, d):
        phase, s = names[number]
        axis = axes[phase]
        h = SIZES[axis] // 2
        sign = (1, -1)[d]
        index = {a: at[a] for a in axes[:phase]}
        index[axis] = shifted(at, axis, -s * sign)
        place = (j, slice(None), *place_of(index, d if s == h else None, first, rows))
        return pltpu.make_async_remote_copy(
            src_ref=full.at[place],
            dst_ref=full.at[place],
            send_sem=send_sem.at[j, c, d],
            recv_sem=recv_sem.at[j, c, number, d],
            device_id=device(at, axis, shifted(at, axis, sign)),
            device_id_type=MESH,
        )

    def action(number):
        def run():
            if number > 0:
                for d in range(2):
                    arriving(number - 1, d).wait_recv()
                for d in range(2):
                    copy(number - 1, d).wait_send()
            if number < len(names):
                for d in range(2):
                    copy(number, d).start()

        return run

    return [action(n) for n in range(len(names) + 1)]


def sum_actions(at, squares_ref, total_ref, boxes, send_sem, recv_sem):
    order = ("z", "x", "y")

    def copies(n):
        axis = order[n]
        base = sum(SIZES[a] - 1 for a in order[:n])
        box = boxes[axis]
        return [
            pltpu.make_async_remote_copy(
                src_ref=box.at[at[axis]],
                dst_ref=box.at[at[axis]],
                send_sem=send_sem.at[base + by - 1],
                recv_sem=recv_sem.at[base + by - 1],
                device_id=device(at, axis, shifted(at, axis, by)),
                device_id_type=MESH,
            )
            for by in range(1, SIZES[axis])
        ]

    def action(n):
        def run():
            if n == 0:
                value = squares_ref[...]
            else:
                for one in copies(n - 1):
                    one.wait()
                box = boxes[order[n - 1]]
                value = box[0]
                for i in range(1, SIZES[order[n - 1]]):
                    value = value + box[i]
            if n == len(order):
                total_ref[...] = value
                return
            boxes[order[n]][at[order[n]]] = value
            for one in copies(n):
                one.start()

        return run

    return [action(n) for n in range(len(order) + 1)]


def gather_kernel(shard_ref, squares_ref, out_ref, total_ref, full, box_x, box_y, box_z, load_sem, out_sem, send_sem, recv_sem, sum_send, sum_recv):
    at = here()
    mine = full.at[:, :, at["x"], at["y"], at["z"]]
    load = pltpu.make_async_copy(shard_ref, mine, load_sem)
    load.start()
    meet(at)
    load.wait()
    sums = sum_actions(at, squares_ref, total_ref, {"x": box_x, "y": box_y, "z": box_z}, sum_send, sum_recv)
    sums[0]()
    streams = {(j, c): gather_steps(j, c) for j in range(3) for c in range(3)}
    events = gather_order(streams)
    actions = {(j, c): gather_actions(j, c, at, full, send_sem, recv_sem) for j, c in streams}
    count = dict.fromkeys(streams, 0)
    left = {j: 3 for j in range(3)}
    outs = [pltpu.make_async_copy(full.at[j], out_ref.at[j], out_sem.at[j]) for j in range(3)]
    summed = 1
    for t, key in events:
        while summed < len(sums) and t > 5.0 * summed:
            sums[summed]()
            summed += 1
        actions[key][count[key]]()
        count[key] += 1
        if count[key] == len(actions[key]):
            left[key[0]] -= 1
            if left[key[0]] == 0:
                outs[key[0]].start()
    for one in outs:
        one.wait()


def gathered(shards, squares):
    sent = 6 * D * FF * 2
    return pl.pallas_call(
        gather_kernel,
        out_shape=(jax.ShapeDtypeStruct((3, 2, 4, 4, 8, SHARD, LANES), BF), jax.ShapeDtypeStruct((8, LANES), F32)),
        in_specs=[pl.BlockSpec(memory_space=pltpu.HBM), pl.BlockSpec(memory_space=pltpu.VMEM)],
        out_specs=[pl.BlockSpec(memory_space=pltpu.HBM), pl.BlockSpec(memory_space=pltpu.VMEM)],
        scratch_shapes=[
            pltpu.VMEM((3, 2, 4, 4, 8, SHARD, LANES), BF),
            pltpu.VMEM((4, 8, LANES), F32),
            pltpu.VMEM((4, 8, LANES), F32),
            pltpu.VMEM((8, 8, LANES), F32),
            pltpu.SemaphoreType.DMA,
            pltpu.SemaphoreType.DMA((3,)),
            pltpu.SemaphoreType.DMA((3, 3, 2)),
            pltpu.SemaphoreType.DMA((3, 3, 8, 2)),
            pltpu.SemaphoreType.DMA((13,)),
            pltpu.SemaphoreType.DMA((13,)),
        ],
        compiler_params=pltpu.CompilerParams(collective_id=1, has_side_effects=True, vmem_limit_bytes=LIMIT),
        cost_estimate=pl.CostEstimate(flops=sent * 100, bytes_accessed=2 * sent, transcendentals=0),
        name="gather",
    )(shards, squares)


def adamw_kernel(total_ref, g_ref, *refs):
    ins, outs, factor_ref = refs[:9], refs[9:18], refs[18]

    @pl.when(jnp.logical_and(pl.program_id(0) == 0, pl.program_id(1) == 0))
    def _():
        mean = jnp.sum(total_ref[...], keepdims=True) * (1.0 / (6 * D * FF))
        factor_ref[...] = jnp.broadcast_to(jnp.minimum(1.0, 0.5 * lax.rsqrt(mean + 1e-30)), factor_ref.shape)

    factor = factor_ref[0:1, :]

    def one(j, g, place):
        w_ref, m_ref, v_ref = ins[3 * j : 3 * j + 3]
        wo_ref, mo_ref, vo_ref = outs[3 * j : 3 * j + 3]
        w = w_ref[place].astype(F32)
        m = 0.9 * m_ref[place] + 0.1 * g
        v = 0.95 * v_ref[place] + 0.05 * g * g
        step = m * lax.rsqrt(v + 1e-8) + 0.1 * w
        wo_ref[place] = (w - 0.02 * step).astype(BF)
        mo_ref[place] = m
        vo_ref[place] = v

    for half in range(PANEL // LANES):
        lanes = pl.ds(half * LANES, LANES)

        def body(i, carry):
            here_rows = pl.ds(pl.multiple_of(half * D + i * 128, 128), 128)
            rows = pl.ds(pl.multiple_of(i * 128, 128), 128)
            for j in (1, 2):
                one(j, g_ref[j, here_rows, :].astype(F32) * factor, (rows, lanes))
            return carry

        lax.fori_loop(0, D // 128, body, 0)
        for i in range(D // 128):
            g = g_ref[0, pl.ds(half * D + i * 128, 128), :].astype(F32) * factor
            one(0, g.T, (lanes, pl.ds(i * 128, 128)))


def adamw(total, g, weights):
    wide = pl.BlockSpec((None, D, PANEL), lambda l, p: (l, 0, p))
    tall = pl.BlockSpec((None, PANEL, D), lambda l, p: (l, p, 0))
    specs = [tall] * 3 + [wide] * 6
    arrays = [a for one in weights for a in one]
    return pl.pallas_call(
        adamw_kernel,
        grid=(2, PANELS),
        out_shape=[jax.ShapeDtypeStruct(a.shape, a.dtype) for a in arrays],
        in_specs=[
            pl.BlockSpec((8, LANES), lambda l, p: (0, 0)),
            pl.BlockSpec((3, None, PANEL // LANES * D, LANES), lambda l, p: (0, 1 - l, p, 0)),
            *specs,
        ],
        out_specs=specs,
        scratch_shapes=[pltpu.VMEM((8, LANES), F32)],
        compiler_params=pltpu.CompilerParams(vmem_limit_bytes=LIMIT, dimension_semantics=("arbitrary", "arbitrary")),
        cost_estimate=pl.CostEstimate(flops=6 * D * FF * 30, bytes_accessed=6 * D * FF * 22, transcendentals=6 * D * FF),
        name="adamw",
    )(total, g, *arrays)


def solution(mesh):
    def step(x, dy, w_gate, w_up, w_down, m_gate, m_up, m_down, v_gate, v_up, v_down):
        xt, ys = row_wise(x[0], dy[0], w_gate, w_up, w_down)
        shards, squares = scattered(xt, ys)
        full, total = gathered(shards, squares)
        new = adamw(
            total,
            full.reshape(3, 2, 128 * SHARD, LANES),
            ((w_down, m_down, v_down), (w_gate, m_gate, v_gate), (w_up, m_up, v_up)),
        )
        return tuple(new[3 * j + which] for which in range(3) for j in (1, 2, 0))

    return jax.shard_map(
        step,
        mesh=mesh,
        in_specs=(P(("rep", "dp"), None, None),) * 2 + (P(None, None, None),) * 9,
        out_specs=(P("rep", None, None),) * 9,
        check_vma=False,
    )
```

```python
import functools

import jax
import jax.numpy as jnp
from jax import lax
from jax.experimental import pallas as pl
from jax.experimental.pallas import tpu as pltpu
from jax.sharding import PartitionSpec as P

BF, F32 = jnp.bfloat16, jnp.float32
MESH = pl.DeviceIdType.MESH
SIZES = {"x": 4, "y": 4, "z": 8}
AXES = ("x", "y", "z")
LANES = 128
SHARD = 128
D, FF, TOKENS = 896, 2304, 2048
PANEL = 256
PANELS = FF // PANEL
LIMIT = 66_900_000
ORDERS = tuple((("z", *second), ("x", "y", "z"), ("y", "x", "z")) for second in (("x", "y"), ("y", "x"), ("x", "y")))
ROWS = ((48, 48, 32), (48, 32, 48), (32, 48, 48))


def colour(j, c):
    return sum(ROWS[j][:c]), ROWS[j][c]


def here():
    d = lax.axis_index("dp")
    return {"x": d // 32, "y": (d // 8) % 4, "z": d % 8}


def device(at, axis, value):
    at = dict(at, **{axis: value})
    return {"dp": (at["x"] * 4 + at["y"]) * 8 + at["z"]}


def shifted(at, axis, by):
    n = SIZES[axis]
    return (at[axis] + (by % n)) % n


def meet(at):
    barrier = pltpu.get_barrier_semaphore()
    peers = [(axis, by) for axis in AXES for by in range(1, SIZES[axis])]
    for axis, by in peers:
        pl.semaphore_signal(barrier, inc=1, device_id=device(at, axis, shifted(at, axis, by)), device_id_type=MESH)
    pl.semaphore_wait(barrier, len(peers))


def place_of(fixed, half, first, rows):
    place, halved = [], half is None
    for a in AXES:
        if a in fixed:
            place.append(fixed[a])
        elif not halved:
            n = SIZES[a] // 2
            place.append(pl.ds(half * n, n))
            halved = True
        else:
            place.append(slice(None))
    begin, size = first, rows
    if not halved:
        one = (rows // 2 + 15) // 16 * 16
        begin, size = (first, one) if half == 0 else (first + one, rows - one)
    return tuple(place) + (pl.ds(begin, size), slice(None))


TB = 512


def dot(a, b):
    return lax.dot_general(a, b, (((1,), (0,)), ((), ())), preferred_element_type=F32)


def dot_t(a, b):
    return lax.dot_general(a, b, (((1,), (1,)), ((), ())), preferred_element_type=F32)


def rows_kernel(x_ref, dy_ref, wg_ref, wu_ref, wd_ref, xt_hbm, ys_hbm, wg, wu, wd, gate0, up0, a_buf, h_buf, xt_ref, ys_ref, load_sem, xt_sem, ys_sem):
    block = pl.program_id(0)
    first, last = block == 0, block == pl.num_programs(0) - 1
    loads = {
        (name, layer): pltpu.make_async_copy(ref.at[layer], buf.at[layer], load_sem.at[n, layer])
        for n, (name, ref, buf) in enumerate((("g", wg_ref, wg), ("u", wu_ref, wu), ("d", wd_ref, wd)))
        for layer in range(2)
    }

    @pl.when(first)
    def _():
        for layer in range(2):
            for name in "gud":
                loads[name, layer].start()

    def need(*which):
        @pl.when(first)
        def _():
            for one in which:
                loads[one].wait()

    tokens = pl.ds(pl.multiple_of(block * TB, TB), TB)

    def xt_out(*at):
        return pltpu.make_async_copy(xt_ref.at[at], xt_hbm.at[(*at, slice(None), tokens)], xt_sem.at[at])

    def ys_out(*at):
        return pltpu.make_async_copy(ys_ref.at[at], ys_hbm.at[(*at, tokens, slice(None))], ys_sem.at[at])

    def free(*outs):
        @pl.when(jnp.logical_not(first))
        def _():
            for one in outs:
                one.wait()

    def scale_of(wide):
        return lax.rsqrt(jnp.mean(wide * wide, -1, keepdims=True) + 1e-6)

    x = x_ref[...].astype(F32)
    a0 = (x * scale_of(x)).astype(BF)
    a_buf[...] = a0
    free(xt_out(1, 1), xt_out(0, 0))
    xt_ref[1, 1] = a0.T
    xt_ref[0, 0] = dy_ref[...].T
    xt_out(1, 1).start()
    xt_out(0, 0).start()
    free(ys_out(1, 0))
    need(("g", 0), ("u", 0))

    def panels(body):
        for p in range(PANELS):
            body(p)

    def at(p):
        return pl.ds(p * PANEL, PANEL)

    def forward0(p):
        gate, up = dot(a_buf[...], wg[0, :, at(p)]), dot(a_buf[...], wu[0, :, at(p)])
        gate0[:, at(p)], up0[:, at(p)] = gate, up
        ys_ref[1, 0, :, at(p)] = (gate * lax.logistic(gate) * up).astype(BF)

    panels(forward0)
    ys_out(1, 0).start()
    need(("d", 0))
    h = x + dot(ys_ref[1, 0], wd[0]).astype(BF).astype(F32)
    h = h.astype(BF).astype(F32)
    h_buf[...] = h
    a1 = (h * scale_of(h)).astype(BF)
    a_buf[...] = a1
    free(xt_out(0, 1))
    xt_ref[0, 1] = a1.T
    xt_out(0, 1).start()
    free(ys_out(0, 0), ys_out(0, 1), ys_out(0, 2))
    need(("g", 1), ("u", 1), ("d", 1))

    def back(d, gate, up):
        d = d.astype(BF).astype(F32)
        s = lax.logistic(gate)
        silu = gate * s
        return (d * up * (s + silu * (1.0 - s))).astype(BF), (d * silu).astype(BF), (silu * up).astype(BF)

    def both1(p):
        gate, up = dot(a_buf[...], wg[1, :, at(p)]), dot(a_buf[...], wu[1, :, at(p)])
        d = dot_t(dy_ref[...], wd[1, at(p), :])
        ys_ref[0, 1, :, at(p)], ys_ref[0, 2, :, at(p)], ys_ref[0, 0, :, at(p)] = back(d, gate, up)

    panels(both1)
    for j in range(3):
        ys_out(0, j).start()
    da = dot_t(ys_ref[0, 1], wg[1]).astype(BF).astype(F32) + dot_t(ys_ref[0, 2], wu[1]).astype(BF).astype(F32)
    da = da.astype(BF).astype(F32)
    h = h_buf[...]
    scale = scale_of(h)
    dh = scale * da - h * (scale * scale * scale * jnp.mean(da * h, -1, keepdims=True))
    dh = (dy_ref[...].astype(F32) + dh.astype(BF).astype(F32)).astype(BF)
    a_buf[...] = dh
    free(xt_out(1, 0))
    xt_ref[1, 0] = dh.T
    xt_out(1, 0).start()
    free(ys_out(1, 1), ys_out(1, 2))

    def back0(p):
        d = dot_t(a_buf[...], wd[0, at(p), :])
        ys_ref[1, 1, :, at(p)], ys_ref[1, 2, :, at(p)], _ = back(d, gate0[:, at(p)], up0[:, at(p)])

    panels(back0)
    for j in (1, 2):
        ys_out(1, j).start()

    @pl.when(last)
    def _():
        for g in range(2):
            for kind in range(2):
                xt_out(g, kind).wait()
            for j in range(3):
                ys_out(g, j).wait()


def row_wise(x, dy, w_gate, w_up, w_down):
    tokens = x.shape[0]
    return pl.pallas_call(
        rows_kernel,
        grid=(tokens // TB,),
        out_shape=(jax.ShapeDtypeStruct((2, 2, D, tokens), BF), jax.ShapeDtypeStruct((2, 3, tokens, FF), BF)),
        in_specs=[pl.BlockSpec((TB, D), lambda i: (i, 0))] * 2 + [pl.BlockSpec(memory_space=pltpu.HBM)] * 3,
        out_specs=[pl.BlockSpec(memory_space=pltpu.HBM)] * 2,
        scratch_shapes=[
            pltpu.VMEM((2, D, FF), BF),
            pltpu.VMEM((2, D, FF), BF),
            pltpu.VMEM((2, FF, D), BF),
            pltpu.VMEM((TB, FF), F32),
            pltpu.VMEM((TB, FF), F32),
            pltpu.VMEM((TB, D), BF),
            pltpu.VMEM((TB, D), F32),
            pltpu.VMEM((2, 2, D, TB), BF),
            pltpu.VMEM((2, 3, TB, FF), BF),
            pltpu.SemaphoreType.DMA((3, 2)),
            pltpu.SemaphoreType.DMA((2, 2)),
            pltpu.SemaphoreType.DMA((2, 3)),
        ],
        compiler_params=pltpu.CompilerParams(vmem_limit_bytes=LIMIT, dimension_semantics=("arbitrary",)),
        cost_estimate=pl.CostEstimate(flops=9 * 2 * tokens * D * FF, bytes_accessed=100_000_000, transcendentals=0),
        name="rows",
    )(x, dy, w_gate, w_up, w_down)


def scatter_actions(j, c, at, own, recv, send_sem, recv_sem, finish):
    first, rows = colour(j, c)
    axes = ORDERS[j][c]

    def add(target, buffers):
        def body(i, carry):
            place = (...,) if i is None else (i,)
            value = target[place].astype(F32)
            for b in buffers:
                value = value + b[place].astype(F32)
            target[place] = value.astype(BF)
            return carry

        if len(target.shape) == 4:
            lax.fori_loop(0, target.shape[0], body, 0)
        else:
            body(None, 0)

    def parts(phase):
        axis = axes[phase]
        h = SIZES[axis] // 2
        fixed = {a: at[a] for a in axes[:phase]}
        buffer = recv[(j * 3 + c) * 3 + phase]
        base = sum(SIZES[a] // 2 for a in axes[:phase])

        def owner(by):
            return dict(fixed, **{axis: shifted(at, axis, by)})

        def slot(s, d):
            index = owner(0)
            if s > 1:
                return (2 * s - 3 + d,)
            place = place_of(index, d, 0, rows)
            return (0,) + tuple(one for a, one in zip(AXES, place[:3], strict=True) if a not in index) + place[3:]

        def copy(g, s, d):
            sign = (1, -1)[d]
            return pltpu.make_async_remote_copy(
                src_ref=own.at[(g, j, *place_of(owner((h - s + 1) * sign), d if s == 1 else None, first, rows))],
                dst_ref=buffer.at[(g, *slot(s, d))],
                send_sem=send_sem.at[g, j, c, d],
                recv_sem=recv_sem.at[g, j, c, base + s - 1, d],
                device_id=device(at, axis, shifted(at, axis, sign)),
                device_id_type=MESH,
            )

        def step(g, s):
            for d in range(2):
                copy(g, s, d).wait_recv()
            if s < h:
                for d in range(2):
                    by = (h - s) * (1, -1)[d]
                    place = place_of(owner(by), d if s == 1 else None, first, rows)
                    add(own.at[(g, j, *place)], [buffer.at[(g, *slot(s, d))]])
            else:
                place = place_of(owner(0), None, first, rows)
                add(own.at[(g, j, *place)], [buffer.at[(g, *slot(s, d))] for d in range(2)])

        return h, copy, step

    def action(number):
        def run(g):
            left, phase = number, 0
            while phase < 3 and left > SIZES[axes[phase]] // 2:
                left -= SIZES[axes[phase]] // 2
                phase += 1
            h, copy, step = parts(phase)
            if left > 0:
                step(g, left)
            before = [copy(g, left, d) for d in range(2)] if left > 0 else []
            if left == h:
                if phase == 2:
                    for one in before:
                        one.wait_send()
                    finish(g, j, c, own.at[(g, j, *place_of(at, None, first, rows))])
                    return
                _, copy, _ = parts(phase + 1)
                left = 0
            for one in before:
                one.wait_send()
            for d in range(2):
                copy(g, left + 1, d).start()

        return run

    return [action(n) for n in range(1 + sum(SIZES[a] // 2 for a in axes))]


SLOTS = (
    (),
    (),
    ((1, 1, 3),),
    ((1, 4, 2),),
    (),
    ((1, 6, 2),),
    (),
    ((1, 8, 2),),
    ((1, 0, 4), (0, 1, 0), (0, 2, 0),),
    ((2, 3, 6), (1, 7, 2),),
    ((1, 5, 3), (0, 0, 0), (2, 2, 6),),
    (),
    ((0, 2, 1), (2, 4, 6),),
    ((1, 1, 4),),
    ((2, 5, 6), (0, 0, 1), (2, 6, 6),),
    ((2, 8, 6), (0, 1, 1),),
    ((2, 7, 6),),
    ((2, 0, 7), (0, 5, 0), (0, 3, 0),),
    ((1, 6, 3),),
    ((0, 4, 0), (1, 4, 3), (1, 8, 3),),
    ((0, 3, 1), (1, 2, 4),),
    ((0, 5, 1), (0, 0, 2),),
    (),
    ((1, 0, 5),),
    (),
    (),
    ((0, 7, 0), (1, 3, 4), (1, 1, 5), (2, 4, 7), (0, 6, 0), (1, 7, 3), (2, 1, 7), (2, 5, 7), (0, 3, 2), (2, 3, 7), (1, 4, 4), (0, 2, 2), (2, 2, 7), (0, 8, 0), (1, 5, 4), (2, 6, 7), (1, 3, 5), (0, 5, 2), (1, 6, 4), (1, 2, 5), (2, 8, 7), (0, 4, 1), (0, 6, 1), (2, 7, 7), (2, 0, 8), (0, 1, 2), (1, 8, 4), (2, 1, 8), (1, 7, 4), (0, 0, 3), (1, 1, 6), (2, 4, 8), (1, 4, 5), (0, 7, 1), (2, 2, 8), (1, 5, 5), (2, 6, 8), (1, 6, 5), (0, 2, 3), (2, 5, 8), (2, 3, 8), (2, 8, 8), (0, 8, 1), (0, 3, 3), (1, 8, 5), (2, 7, 8), (1, 7, 5), (1, 0, 6),),
    (),
)


def scatter_kernel(xt_ref, ys_ref, shard_ref, squares_ref, own, *refs):
    recv, refs = refs[:27], refs[27:]
    xbuf, ybuf, x_sem, y_sem, send_sem, recv_sem = refs
    at = here()
    total = 3 * PANELS

    def load_x(g, kind):
        return pltpu.make_async_copy(xt_ref.at[g, kind], xbuf.at[kind], x_sem.at[kind])

    def load_y(g, n):
        lanes = pl.ds(pl.multiple_of((n % PANELS) * PANEL, PANEL), PANEL)
        return pltpu.make_async_copy(ys_ref.at[g, n // PANELS, :, lanes], ybuf.at[n % 3], y_sem.at[n % 3])

    load_x(0, 0).start()
    load_y(0, 0).start()
    load_y(0, 1).start()
    load_x(0, 1).start()
    squares_ref[...] = jnp.zeros_like(squares_ref)
    for g in range(2):
        for j in range(3):
            for z in (6, 7):
                own[g, j, 3, 3, z] = jnp.zeros((SHARD, LANES), BF)
    meet(at)

    def finish(g, j, c, region):
        first, rows = colour(j, c)
        value = region[...]
        shard_ref[j, g, pl.ds(first, rows), :] = value
        wide = value.astype(F32)
        squares_ref[...] += jnp.sum((wide * wide).reshape(rows // 8, 8, LANES), axis=0)

    actions = [scatter_actions(j, c, at, own, recv, send_sem, recv_sem, finish) for j in range(3) for c in range(3)]
    rounds = 2 + max(late for todo in SLOTS for late, _, _ in todo)

    def group(i, carry):
        def slot(n, carry):
            @pl.when(jnp.logical_and(n < total, i < 2))
            def _():
                j, p = n // PANELS, n % PANELS
                kind = jnp.minimum(j, 1)

                @pl.when(n == 0)
                def _():
                    load_x(i, 0).wait()

                @pl.when(n == PANELS)
                def _():
                    load_x(i, 1).wait()

                    @pl.when(i < 1)
                    def _():
                        load_x(i + 1, 0).start()

                load_y(i, n).wait()

                @pl.when(n + 2 < total)
                def _():
                    load_y(i, n + 2).start()

                @pl.when(jnp.logical_and(n + 2 >= total, i < 1))
                def _():
                    load_y(i + 1, n + 2 - total).start()

                out = dot(xbuf[kind], ybuf[n % 3])
                for half in range(PANEL // LANES):
                    for b in range(D // SHARD):
                        d = (2 * p + half) * (D // SHARD) + b
                        block = out[b * SHARD : (b + 1) * SHARD, half * LANES : (half + 1) * LANES]
                        own[i, j, d // 32, (d // 8) % 4, d % 8] = block.astype(BF)

                @pl.when(jnp.logical_and(n == total - 1, i < 1))
                def _():
                    load_x(i + 1, 1).start()

            def serve(todo):
                for late, key, which in todo:
                    pl.when(jnp.logical_and(i >= late, i < 2 + late))(functools.partial(actions[key][which], i - late))

            def some(low):
                for number in range(low, min(low + 5, len(SLOTS))):
                    if SLOTS[number]:
                        pl.when(n == number)(functools.partial(serve, SLOTS[number]))

            for low in range(0, len(SLOTS), 5):
                pl.when(n // 5 == low // 5)(functools.partial(some, low))
            return carry

        lax.fori_loop(0, total + 1, slot, 0)
        return carry

    lax.fori_loop(0, rounds, group, 0)


def recv_shapes():
    shapes = []
    for j in range(3):
        for c in range(3):
            for phase in range(3):
                axes = ORDERS[j][c]
                left = tuple(SIZES[a] for a in AXES if a not in axes[: phase + 1])
                shapes.append(pltpu.VMEM((2, SIZES[axes[phase]] - 1, *left, ROWS[j][c], LANES), BF))
    return shapes


def scattered(xt, ys):
    sent = 6 * D * FF * 2
    return pl.pallas_call(
        scatter_kernel,
        out_shape=(jax.ShapeDtypeStruct((3, 2, SHARD, LANES), BF), jax.ShapeDtypeStruct((8, LANES), F32)),
        in_specs=[pl.BlockSpec(memory_space=pltpu.HBM)] * 2,
        out_specs=[pl.BlockSpec(memory_space=pltpu.VMEM)] * 2,
        scratch_shapes=[
            pltpu.VMEM((2, 3, 4, 4, 8, SHARD, LANES), BF),
            *recv_shapes(),
            pltpu.VMEM((2, D, TOKENS), BF),
            pltpu.VMEM((3, TOKENS, PANEL), BF),
            pltpu.SemaphoreType.DMA((2,)),
            pltpu.SemaphoreType.DMA((3,)),
            pltpu.SemaphoreType.DMA((2, 3, 3, 2)),
            pltpu.SemaphoreType.DMA((2, 3, 3, 8, 2)),
        ],
        compiler_params=pltpu.CompilerParams(collective_id=0, has_side_effects=True, vmem_limit_bytes=LIMIT),
        cost_estimate=pl.CostEstimate(flops=6 * 2 * TOKENS * D * FF, bytes_accessed=3 * sent, transcendentals=0),
        name="scatter",
    )(xt, ys)


def gather_actions(j, c, at, full, send_sem, recv_sem):
    first, rows = colour(j, c)
    axes = ORDERS[j][c]
    names = []
    for phase in (2, 1, 0):
        for s in range(1, SIZES[axes[phase]] // 2 + 1):
            names.append((phase, s))

    def copy(number, d):
        phase, s = names[number]
        axis = axes[phase]
        h = SIZES[axis] // 2
        sign = (1, -1)[d]
        index = {a: at[a] for a in axes[:phase]}
        index[axis] = shifted(at, axis, -(s - 1) * sign)
        place = (j, slice(None), *place_of(index, d if s == h else None, first, rows))
        return pltpu.make_async_remote_copy(
            src_ref=full.at[place],
            dst_ref=full.at[place],
            send_sem=send_sem.at[j, c, d],
            recv_sem=recv_sem.at[j, c, number, d],
            device_id=device(at, axis, shifted(at, axis, sign)),
            device_id_type=MESH,
        )

    def arriving(number, d):
        phase, s = names[number]
        axis = axes[phase]
        h = SIZES[axis] // 2
        sign = (1, -1)[d]
        index = {a: at[a] for a in axes[:phase]}
        index[axis] = shifted(at, axis, -s * sign)
        place = (j, slice(None), *place_of(index, d if s == h else None, first, rows))
        return pltpu.make_async_remote_copy(
            src_ref=full.at[place],
            dst_ref=full.at[place],
            send_sem=send_sem.at[j, c, d],
            recv_sem=recv_sem.at[j, c, number, d],
            device_id=device(at, axis, shifted(at, axis, sign)),
            device_id_type=MESH,
        )

    def action(number):
        def run():
            if number > 0:
                for d in range(2):
                    arriving(number - 1, d).wait_recv()
                for d in range(2):
                    copy(number - 1, d).wait_send()
            if number < len(names):
                for d in range(2):
                    copy(number, d).start()

        return run

    return [action(n) for n in range(len(names) + 1)]


GATHER = (
    *(4, 6, 2, 3, 7, 5, 0, 4, 6, 2, 3, 7, 5, 0, 4, 6, 2, 3, 1, 8, 7, 0, 4, 2, 5, 1, 8),
    *(6, 7, 4, 2, 5, 8, 1, 0, 7, 3, 5, 8, 4, 1, 6, 2, 8, 1, 5, 0, 7, 4, 3, 2, 1, 7, 8),
    *(5, 0, 1, 2, 6, 3, 8, 5, 7, 6, 3, 0, 6, 1, 0, 2, 4, 3, 8, 6, 3, 5, 7, 0, 1, 8, 4),
)


def sum_actions(at, squares_ref, total_ref, boxes, send_sem, recv_sem):
    order = ("z", "x", "y")

    def copies(n):
        axis = order[n]
        base = sum(SIZES[a] - 1 for a in order[:n])
        box = boxes[axis]
        return [
            pltpu.make_async_remote_copy(
                src_ref=box.at[at[axis]],
                dst_ref=box.at[at[axis]],
                send_sem=send_sem.at[base + by - 1],
                recv_sem=recv_sem.at[base + by - 1],
                device_id=device(at, axis, shifted(at, axis, by)),
                device_id_type=MESH,
            )
            for by in range(1, SIZES[axis])
        ]

    def action(n):
        def run():
            if n == 0:
                value = squares_ref[...]
            else:
                for one in copies(n - 1):
                    one.wait()
                box = boxes[order[n - 1]]
                value = box[0]
                for i in range(1, SIZES[order[n - 1]]):
                    value = value + box[i]
            if n == len(order):
                total_ref[...] = value
                return
            boxes[order[n]][at[order[n]]] = value
            for one in copies(n):
                one.start()

        return run

    return [action(n) for n in range(len(order) + 1)]


def gather_kernel(shard_ref, squares_ref, out_ref, total_ref, full, box_x, box_y, box_z, load_sem, out_sem, send_sem, recv_sem, sum_send, sum_recv):
    at = here()
    mine = full.at[:, :, at["x"], at["y"], at["z"]]
    load = pltpu.make_async_copy(shard_ref, mine, load_sem)
    load.start()
    meet(at)
    load.wait()
    sums = sum_actions(at, squares_ref, total_ref, {"x": box_x, "y": box_y, "z": box_z}, sum_send, sum_recv)
    sums[0]()
    actions = [gather_actions(j, c, at, full, send_sem, recv_sem) for j in range(3) for c in range(3)]
    count = [0] * 9
    left = {j: 3 for j in range(3)}
    outs = [pltpu.make_async_copy(full.at[j], out_ref.at[j], out_sem.at[j]) for j in range(3)]
    summed = 1
    for number, key in enumerate(GATHER):
        if number in (18, 24, 30):
            sums[summed]()
            summed += 1
        actions[key][count[key]]()
        count[key] += 1
        if count[key] == len(actions[key]):
            left[key // 3] -= 1
            if left[key // 3] == 0:
                outs[key // 3].start()
    for one in outs:
        one.wait()


def gathered(shards, squares):
    sent = 6 * D * FF * 2
    return pl.pallas_call(
        gather_kernel,
        out_shape=(jax.ShapeDtypeStruct((3, 2, 4, 4, 8, SHARD, LANES), BF), jax.ShapeDtypeStruct((8, LANES), F32)),
        in_specs=[pl.BlockSpec(memory_space=pltpu.HBM), pl.BlockSpec(memory_space=pltpu.VMEM)],
        out_specs=[pl.BlockSpec(memory_space=pltpu.HBM), pl.BlockSpec(memory_space=pltpu.VMEM)],
        scratch_shapes=[
            pltpu.VMEM((3, 2, 4, 4, 8, SHARD, LANES), BF),
            pltpu.VMEM((4, 8, LANES), F32),
            pltpu.VMEM((4, 8, LANES), F32),
            pltpu.VMEM((8, 8, LANES), F32),
            pltpu.SemaphoreType.DMA,
            pltpu.SemaphoreType.DMA((3,)),
            pltpu.SemaphoreType.DMA((3, 3, 2)),
            pltpu.SemaphoreType.DMA((3, 3, 8, 2)),
            pltpu.SemaphoreType.DMA((13,)),
            pltpu.SemaphoreType.DMA((13,)),
        ],
        compiler_params=pltpu.CompilerParams(collective_id=1, has_side_effects=True, vmem_limit_bytes=LIMIT),
        cost_estimate=pl.CostEstimate(flops=sent * 100, bytes_accessed=2 * sent, transcendentals=0),
        name="gather",
    )(shards, squares)


def adamw_kernel(total_ref, g_ref, *refs):
    ins, outs, factor_ref = refs[:9], refs[9:18], refs[18]

    @pl.when(jnp.logical_and(pl.program_id(0) == 0, pl.program_id(1) == 0))
    def _():
        mean = jnp.sum(total_ref[...], keepdims=True) * (1.0 / (6 * D * FF))
        factor_ref[...] = jnp.broadcast_to(jnp.minimum(1.0, 0.5 * lax.rsqrt(mean + 1e-30)), factor_ref.shape)

    factor = factor_ref[0:1, :]

    def one(j, g, place):
        w_ref, m_ref, v_ref = ins[3 * j : 3 * j + 3]
        wo_ref, mo_ref, vo_ref = outs[3 * j : 3 * j + 3]
        w = w_ref[place].astype(F32)
        m = 0.9 * m_ref[place] + 0.1 * g
        v = 0.95 * v_ref[place] + 0.05 * g * g
        step = m * lax.rsqrt(v + 1e-8) + 0.1 * w
        wo_ref[place] = (w - 0.02 * step).astype(BF)
        mo_ref[place] = m
        vo_ref[place] = v

    for half in range(PANEL // LANES):
        lanes = pl.ds(half * LANES, LANES)

        def body(i, carry):
            here_rows = pl.ds(pl.multiple_of(half * D + i * 128, 128), 128)
            rows = pl.ds(pl.multiple_of(i * 128, 128), 128)
            for j in (1, 2):
                one(j, g_ref[j, here_rows, :].astype(F32) * factor, (rows, lanes))
            return carry

        lax.fori_loop(0, D // 128, body, 0)
        for i in range(D // 128):
            g = g_ref[0, pl.ds(half * D + i * 128, 128), :].astype(F32) * factor
            one(0, g.T, (lanes, pl.ds(i * 128, 128)))


def adamw(total, g, weights):
    wide = pl.BlockSpec((None, D, PANEL), lambda l, p: (l, 0, p))
    tall = pl.BlockSpec((None, PANEL, D), lambda l, p: (l, p, 0))
    specs = [tall] * 3 + [wide] * 6
    arrays = [a for one in weights for a in one]
    return pl.pallas_call(
        adamw_kernel,
        grid=(2, PANELS),
        out_shape=[jax.ShapeDtypeStruct(a.shape, a.dtype) for a in arrays],
        in_specs=[
            pl.BlockSpec((8, LANES), lambda l, p: (0, 0)),
            pl.BlockSpec((3, None, PANEL // LANES * D, LANES), lambda l, p: (0, 1 - l, p, 0)),
            *specs,
        ],
        out_specs=specs,
        scratch_shapes=[pltpu.VMEM((8, LANES), F32)],
        compiler_params=pltpu.CompilerParams(vmem_limit_bytes=LIMIT, dimension_semantics=("arbitrary", "arbitrary")),
        cost_estimate=pl.CostEstimate(flops=6 * D * FF * 30, bytes_accessed=6 * D * FF * 22, transcendentals=6 * D * FF),
        name="adamw",
    )(total, g, *arrays)


def solution(mesh):
    def step(x, dy, w_gate, w_up, w_down, m_gate, m_up, m_down, v_gate, v_up, v_down):
        xt, ys = row_wise(x[0], dy[0], w_gate, w_up, w_down)
        shards, squares = scattered(xt, ys)
        full, total = gathered(shards, squares)
        new = adamw(
            total,
            full.reshape(3, 2, 128 * SHARD, LANES),
            ((w_down, m_down, v_down), (w_gate, m_gate, v_gate), (w_up, m_up, v_up)),
        )
        return tuple(new[3 * j + which] for which in range(3) for j in (1, 2, 0))

    return jax.shard_map(
        step,
        mesh=mesh,
        in_specs=(P(("rep", "dp"), None, None),) * 2 + (P(None, None, None),) * 9,
        out_specs=(P("rep", None, None),) * 9,
        check_vma=False,
    )
```

```python
import functools

import jax
import jax.numpy as jnp
from jax import lax
from jax.experimental import pallas as pl
from jax.experimental.pallas import tpu as pltpu
from jax.sharding import PartitionSpec as P

BF, F32 = jnp.bfloat16, jnp.float32
MESH = pl.DeviceIdType.MESH
SIZES = {"x": 4, "y": 4, "z": 8}
AXES = ("x", "y", "z")
LANES = 128
SHARD = 128
D, FF, TOKENS = 896, 2304, 2048
PANEL = 256
PANELS = FF // PANEL
LIMIT = 66_900_000
ORDERS = tuple((("z", *second), ("x", "y", "z"), ("y", "x", "z")) for second in (("x", "y"), ("y", "x"), ("x", "y")))
ROWS = ((48, 48, 32), (48, 32, 48), (32, 48, 48))


def colour(j, c):
    return sum(ROWS[j][:c]), ROWS[j][c]


def here():
    d = lax.axis_index("dp")
    return {"x": d // 32, "y": (d // 8) % 4, "z": d % 8}


def device(at, axis, value):
    at = dict(at, **{axis: value})
    return {"dp": (at["x"] * 4 + at["y"]) * 8 + at["z"]}


def shifted(at, axis, by):
    n = SIZES[axis]
    return (at[axis] + (by % n)) % n


def meet(at):
    barrier = pltpu.get_barrier_semaphore()
    peers = [(axis, by) for axis in AXES for by in range(1, SIZES[axis])]
    for axis, by in peers:
        pl.semaphore_signal(barrier, inc=1, device_id=device(at, axis, shifted(at, axis, by)), device_id_type=MESH)
    pl.semaphore_wait(barrier, len(peers))


def place_of(fixed, half, first, rows):
    place, halved = [], half is None
    for a in AXES:
        if a in fixed:
            place.append(fixed[a])
        elif not halved:
            n = SIZES[a] // 2
            place.append(pl.ds(half * n, n))
            halved = True
        else:
            place.append(slice(None))
    begin, size = first, rows
    if not halved:
        one = (rows // 2 + 15) // 16 * 16
        begin, size = (first, one) if half == 0 else (first + one, rows - one)
    return tuple(place) + (pl.ds(begin, size), slice(None))


RATE, LATENCY, SERVE = 45.0e3, 2.2, 0.3


def bytes_of(j, c, phase, part):
    size = SHARD * SHARD * LANES * 2 * ROWS[j][c] // SHARD
    for axis in ORDERS[j][c][: phase + 1]:
        size //= SIZES[axis]
    return size * part


def gather_steps(j, c):
    out = []
    for phase, axis in reversed(list(enumerate(ORDERS[j][c]))):
        h = SIZES[axis] // 2
        for s in range(1, h + 1):
            out.append((axis, 2 * bytes_of(j, c, phase, 0.5 if s == h else 1)))
    return out


def gather_order(streams):
    free = dict.fromkeys(AXES, 0.0)
    arrival, position = {}, {}
    now, out = 0.0, []
    waiting = list(streams)

    def send(key, at):
        axis, size = streams[key][at]
        free[axis] = max(now, free[axis]) + size / RATE
        arrival[key], position[key] = free[axis] + LATENCY, at

    while waiting or arrival:
        choices = sorted((t, key) for key, t in arrival.items())
        start = next((key for key in waiting if free[streams[key][0][0]] < now + 3.0), None)
        if start is not None:
            now += SERVE
            out.append((now, start))
            waiting.remove(start)
            send(start, 0)
        elif choices and choices[0][0] <= now:
            key = choices[0][1]
            now += SERVE
            out.append((now, key))
            del arrival[key]
            if position[key] + 1 < len(streams[key]):
                send(key, position[key] + 1)
        else:
            later = [choices[0][0]] if choices else []
            later += [free[streams[key][0][0]] - 3.0 for key in waiting]
            now = max(now + 0.01, min(later))
    return out


TB = 512


def dot(a, b):
    return lax.dot_general(a, b, (((1,), (0,)), ((), ())), preferred_element_type=F32)


def dot_t(a, b):
    return lax.dot_general(a, b, (((1,), (1,)), ((), ())), preferred_element_type=F32)


def rows_kernel(x_ref, dy_ref, wg_ref, wu_ref, wd_ref, xt_hbm, ys_hbm, wg, wu, wd, gate0, up0, a_buf, h_buf, xt_ref, ys_ref, load_sem, xt_sem, ys_sem):
    block = pl.program_id(0)
    first, last = block == 0, block == pl.num_programs(0) - 1
    loads = {
        (name, layer): pltpu.make_async_copy(ref.at[layer], buf.at[layer], load_sem.at[n, layer])
        for n, (name, ref, buf) in enumerate((("g", wg_ref, wg), ("u", wu_ref, wu), ("d", wd_ref, wd)))
        for layer in range(2)
    }

    @pl.when(first)
    def _():
        for layer in range(2):
            for name in "gud":
                loads[name, layer].start()

    def need(*which):
        @pl.when(first)
        def _():
            for one in which:
                loads[one].wait()

    tokens = pl.ds(pl.multiple_of(block * TB, TB), TB)

    def xt_out(*at):
        return pltpu.make_async_copy(xt_ref.at[at], xt_hbm.at[(*at, slice(None), tokens)], xt_sem.at[at])

    def ys_out(*at):
        return pltpu.make_async_copy(ys_ref.at[at], ys_hbm.at[(*at, tokens, slice(None))], ys_sem.at[at])

    def free(*outs):
        @pl.when(jnp.logical_not(first))
        def _():
            for one in outs:
                one.wait()

    def scale_of(wide):
        return lax.rsqrt(jnp.mean(wide * wide, -1, keepdims=True) + 1e-6)

    x = x_ref[...].astype(F32)
    a0 = (x * scale_of(x)).astype(BF)
    a_buf[...] = a0
    free(xt_out(1, 1), xt_out(0, 0))
    xt_ref[1, 1] = a0.T
    xt_ref[0, 0] = dy_ref[...].T
    xt_out(1, 1).start()
    xt_out(0, 0).start()
    free(ys_out(1, 0))
    need(("g", 0), ("u", 0))

    def panels(body):
        for p in range(PANELS):
            body(p)

    def at(p):
        return pl.ds(p * PANEL, PANEL)

    def forward0(p):
        gate, up = dot(a_buf[...], wg[0, :, at(p)]), dot(a_buf[...], wu[0, :, at(p)])
        gate0[:, at(p)], up0[:, at(p)] = gate, up
        ys_ref[1, 0, :, at(p)] = (gate * lax.logistic(gate) * up).astype(BF)

    panels(forward0)
    ys_out(1, 0).start()
    need(("d", 0))
    h = x + dot(ys_ref[1, 0], wd[0]).astype(BF).astype(F32)
    h = h.astype(BF).astype(F32)
    h_buf[...] = h
    a1 = (h * scale_of(h)).astype(BF)
    a_buf[...] = a1
    free(xt_out(0, 1))
    xt_ref[0, 1] = a1.T
    xt_out(0, 1).start()
    free(ys_out(0, 0), ys_out(0, 1), ys_out(0, 2))
    need(("g", 1), ("u", 1), ("d", 1))

    def back(d, gate, up):
        d = d.astype(BF).astype(F32)
        s = lax.logistic(gate)
        silu = gate * s
        return (d * up * (s + silu * (1.0 - s))).astype(BF), (d * silu).astype(BF), (silu * up).astype(BF)

    def both1(p):
        gate, up = dot(a_buf[...], wg[1, :, at(p)]), dot(a_buf[...], wu[1, :, at(p)])
        d = dot_t(dy_ref[...], wd[1, at(p), :])
        ys_ref[0, 1, :, at(p)], ys_ref[0, 2, :, at(p)], ys_ref[0, 0, :, at(p)] = back(d, gate, up)

    panels(both1)
    for j in range(3):
        ys_out(0, j).start()
    da = dot_t(ys_ref[0, 1], wg[1]).astype(BF).astype(F32) + dot_t(ys_ref[0, 2], wu[1]).astype(BF).astype(F32)
    da = da.astype(BF).astype(F32)
    h = h_buf[...]
    scale = scale_of(h)
    dh = scale * da - h * (scale * scale * scale * jnp.mean(da * h, -1, keepdims=True))
    dh = (dy_ref[...].astype(F32) + dh.astype(BF).astype(F32)).astype(BF)
    a_buf[...] = dh
    free(xt_out(1, 0))
    xt_ref[1, 0] = dh.T
    xt_out(1, 0).start()
    free(ys_out(1, 1), ys_out(1, 2))

    def back0(p):
        d = dot_t(a_buf[...], wd[0, at(p), :])
        ys_ref[1, 1, :, at(p)], ys_ref[1, 2, :, at(p)], _ = back(d, gate0[:, at(p)], up0[:, at(p)])

    panels(back0)
    for j in (1, 2):
        ys_out(1, j).start()

    @pl.when(last)
    def _():
        for g in range(2):
            for kind in range(2):
                xt_out(g, kind).wait()
            for j in range(3):
                ys_out(g, j).wait()


def row_wise(x, dy, w_gate, w_up, w_down):
    tokens = x.shape[0]
    return pl.pallas_call(
        rows_kernel,
        grid=(tokens // TB,),
        out_shape=(jax.ShapeDtypeStruct((2, 2, D, tokens), BF), jax.ShapeDtypeStruct((2, 3, tokens, FF), BF)),
        in_specs=[pl.BlockSpec((TB, D), lambda i: (i, 0))] * 2 + [pl.BlockSpec(memory_space=pltpu.HBM)] * 3,
        out_specs=[pl.BlockSpec(memory_space=pltpu.HBM)] * 2,
        scratch_shapes=[
            pltpu.VMEM((2, D, FF), BF),
            pltpu.VMEM((2, D, FF), BF),
            pltpu.VMEM((2, FF, D), BF),
            pltpu.VMEM((TB, FF), F32),
            pltpu.VMEM((TB, FF), F32),
            pltpu.VMEM((TB, D), BF),
            pltpu.VMEM((TB, D), F32),
            pltpu.VMEM((2, 2, D, TB), BF),
            pltpu.VMEM((2, 3, TB, FF), BF),
            pltpu.SemaphoreType.DMA((3, 2)),
            pltpu.SemaphoreType.DMA((2, 2)),
            pltpu.SemaphoreType.DMA((2, 3)),
        ],
        compiler_params=pltpu.CompilerParams(vmem_limit_bytes=LIMIT, dimension_semantics=("arbitrary",)),
        cost_estimate=pl.CostEstimate(flops=9 * 2 * tokens * D * FF, bytes_accessed=100_000_000, transcendentals=0),
        name="rows",
    )(x, dy, w_gate, w_up, w_down)


def scatter_actions(j, c, at, own, recv, send_sem, recv_sem, finish):
    first, rows = colour(j, c)
    axes = ORDERS[j][c]

    def add(target, buffers):
        def body(i, carry):
            place = (...,) if i is None else (i,)
            value = target[place].astype(F32)
            for b in buffers:
                value = value + b[place].astype(F32)
            target[place] = value.astype(BF)
            return carry

        if len(target.shape) == 4:
            lax.fori_loop(0, target.shape[0], body, 0)
        else:
            body(None, 0)

    def parts(phase):
        axis = axes[phase]
        h = SIZES[axis] // 2
        fixed = {a: at[a] for a in axes[:phase]}
        buffer = recv[(j * 3 + c) * 3 + phase]
        base = sum(SIZES[a] // 2 for a in axes[:phase])

        def owner(by):
            return dict(fixed, **{axis: shifted(at, axis, by)})

        def slot(s, d):
            index = owner(0)
            if s > 1:
                return (2 * s - 3 + d,)
            place = place_of(index, d, 0, rows)
            return (0,) + tuple(one for a, one in zip(AXES, place[:3], strict=True) if a not in index) + place[3:]

        def copy(g, s, d):
            sign = (1, -1)[d]
            return pltpu.make_async_remote_copy(
                src_ref=own.at[(g, j, *place_of(owner((h - s + 1) * sign), d if s == 1 else None, first, rows))],
                dst_ref=buffer.at[(g, *slot(s, d))],
                send_sem=send_sem.at[g, j, c, d],
                recv_sem=recv_sem.at[g, j, c, base + s - 1, d],
                device_id=device(at, axis, shifted(at, axis, sign)),
                device_id_type=MESH,
            )

        def step(g, s):
            for d in range(2):
                copy(g, s, d).wait_recv()
            if s < h:
                for d in range(2):
                    by = (h - s) * (1, -1)[d]
                    place = place_of(owner(by), d if s == 1 else None, first, rows)
                    add(own.at[(g, j, *place)], [buffer.at[(g, *slot(s, d))]])
            else:
                place = place_of(owner(0), None, first, rows)
                add(own.at[(g, j, *place)], [buffer.at[(g, *slot(s, d))] for d in range(2)])

        return h, copy, step

    def action(number):
        def run(g):
            left, phase = number, 0
            while phase < 3 and left > SIZES[axes[phase]] // 2:
                left -= SIZES[axes[phase]] // 2
                phase += 1
            h, copy, step = parts(phase)
            if left > 0:
                step(g, left)
            before = [copy(g, left, d) for d in range(2)] if left > 0 else []
            if left == h:
                if phase == 2:
                    for one in before:
                        one.wait_send()
                    finish(g, j, c, own.at[(g, j, *place_of(at, None, first, rows))])
                    return
                _, copy, _ = parts(phase + 1)
                left = 0
            for one in before:
                one.wait_send()
            for d in range(2):
                copy(g, left + 1, d).start()

        return run

    return [action(n) for n in range(1 + sum(SIZES[a] // 2 for a in axes))]


SLOTS = (
    ((2, 7, 5), (2, 8, 5), (2, 1, 6), (2, 4, 6), (1, 7, 1), (1, 3, 2),),
    ((1, 6, 2), (1, 8, 1), (1, 4, 2), (2, 5, 6),),
    ((0, 2, 0), (0, 1, 0), (0, 0, 0), (1, 0, 4), (2, 0, 6),),
    ((2, 2, 6), (1, 3, 3), (2, 6, 6),),
    ((1, 5, 2), (2, 7, 6), (1, 2, 3), (0, 0, 1), (1, 7, 2), (1, 1, 3), (2, 3, 6), (0, 1, 1),),
    ((0, 5, 0), (0, 3, 0), (0, 2, 1),),
    ((1, 6, 3), (1, 8, 2), (1, 5, 3), (0, 0, 2), (2, 8, 6), (1, 4, 3),),
    ((1, 7, 3), (2, 4, 7), (0, 4, 0),),
    ((1, 8, 3), (2, 1, 7), (2, 2, 7), (2, 5, 7), (2, 6, 7), (0, 8, 0), (1, 2, 4), (2, 0, 7), (1, 1, 4), (0, 6, 0), (1, 3, 4), (2, 7, 7), (1, 4, 4), (1, 6, 4), (1, 5, 4), (0, 7, 0), (2, 3, 7), (2, 8, 7), (0, 3, 1), (0, 5, 1), (2, 1, 8), (0, 1, 2), (2, 2, 8), (1, 0, 5), (1, 2, 5), (2, 5, 8), (1, 1, 5), (1, 7, 4), (1, 8, 4), (1, 4, 5), (2, 4, 8), (2, 0, 8), (1, 5, 5), (0, 4, 1), (2, 6, 8), (1, 6, 5), (0, 2, 2), (0, 6, 1), (1, 3, 5), (0, 0, 3), (2, 7, 8), (2, 3, 8), (2, 8, 8),),
    (),
)


def scatter_kernel(xt_ref, ys_ref, shard_ref, squares_ref, own, *refs):
    recv, refs = refs[:27], refs[27:]
    xbuf, ybuf, x_sem, y_sem, send_sem, recv_sem = refs
    at = here()
    total = PANELS

    def load_x(g, kind):
        return pltpu.make_async_copy(xt_ref.at[g, kind], xbuf.at[kind], x_sem.at[kind])

    def load_y(g, n):
        copies = []
        for q in range(3):
            lanes = pl.ds(pl.multiple_of((n % 3) * (3 * PANEL) + q * PANEL, PANEL), PANEL)
            copies.append(pltpu.make_async_copy(ys_ref.at[g, n // 3, :, lanes], ybuf.at[(g + n) % 2, q], y_sem.at[(g + n) % 2, q]))
        return copies

    load_x(0, 0).start()
    for one in load_y(0, 0):
        one.start()
    load_x(0, 1).start()
    squares_ref[...] = jnp.zeros_like(squares_ref)
    for g in range(2):
        for j in range(3):
            for z in (6, 7):
                own[g, j, 3, 3, z] = jnp.zeros((SHARD, LANES), BF)
    meet(at)

    def finish(g, j, c, region):
        first, rows = colour(j, c)
        value = region[...]
        shard_ref[j, g, pl.ds(first, rows), :] = value
        wide = value.astype(F32)
        squares_ref[...] += jnp.sum((wide * wide).reshape(rows // 8, 8, LANES), axis=0)

    actions = [scatter_actions(j, c, at, own, recv, send_sem, recv_sem, finish) for j in range(3) for c in range(3)]
    rounds = 2 + max(late for todo in SLOTS for late, _, _ in todo)

    def group(i, carry):
        def slot(n, carry):
            @pl.when(jnp.logical_and(n < total, i < 2))
            def _():
                j = n // 3
                kind = jnp.minimum(j, 1)

                @pl.when(n + 1 < total)
                def _():
                    for one in load_y(i, n + 1):
                        one.start()

                @pl.when(n == 0)
                def _():
                    load_x(i, 0).wait()

                @pl.when(n == 3)
                def _():
                    load_x(i, 1).wait()

                    @pl.when(i < 1)
                    def _():
                        load_x(i + 1, 0).start()

                for one in load_y(i, n):
                    one.wait()
                for q in range(3):
                    out = dot(xbuf[kind], ybuf[(i + n) % 2, q])
                    for half in range(PANEL // LANES):
                        for b in range(D // SHARD):
                            d = (2 * (3 * (n % 3) + q) + half) * (D // SHARD) + b
                            block = out[b * SHARD : (b + 1) * SHARD, half * LANES : (half + 1) * LANES]
                            own[i, j, d // 32, (d // 8) % 4, d % 8] = block.astype(BF)

                @pl.when(jnp.logical_and(n == total - 1, i < 1))
                def _():
                    load_x(i + 1, 1).start()
                    for one in load_y(i + 1, 0):
                        one.start()

            def serve(todo):
                for late, key, which in todo:
                    pl.when(jnp.logical_and(i >= late, i < 2 + late))(functools.partial(actions[key][which], i - late))

            for number, todo in enumerate(SLOTS):
                if todo:
                    pl.when(n == number)(functools.partial(serve, todo))
            return carry

        lax.fori_loop(0, total + 1, slot, 0)
        return carry

    lax.fori_loop(0, rounds, group, 0)


def recv_shapes():
    shapes = []
    for j in range(3):
        for c in range(3):
            for phase in range(3):
                axes = ORDERS[j][c]
                left = tuple(SIZES[a] for a in AXES if a not in axes[: phase + 1])
                shapes.append(pltpu.VMEM((2, SIZES[axes[phase]] - 1, *left, ROWS[j][c], LANES), BF))
    return shapes


def scattered(xt, ys):
    sent = 6 * D * FF * 2
    return pl.pallas_call(
        scatter_kernel,
        out_shape=(jax.ShapeDtypeStruct((3, 2, SHARD, LANES), BF), jax.ShapeDtypeStruct((8, LANES), F32)),
        in_specs=[pl.BlockSpec(memory_space=pltpu.HBM)] * 2,
        out_specs=[pl.BlockSpec(memory_space=pltpu.VMEM)] * 2,
        scratch_shapes=[
            pltpu.VMEM((2, 3, 4, 4, 8, SHARD, LANES), BF),
            *recv_shapes(),
            pltpu.VMEM((2, D, TOKENS), BF),
            pltpu.VMEM((2, 3, TOKENS, PANEL), BF),
            pltpu.SemaphoreType.DMA((2,)),
            pltpu.SemaphoreType.DMA((2, 3)),
            pltpu.SemaphoreType.DMA((2, 3, 3, 2)),
            pltpu.SemaphoreType.DMA((2, 3, 3, 8, 2)),
        ],
        compiler_params=pltpu.CompilerParams(collective_id=0, has_side_effects=True, vmem_limit_bytes=LIMIT),
        cost_estimate=pl.CostEstimate(flops=6 * 2 * TOKENS * D * FF, bytes_accessed=3 * sent, transcendentals=0),
        name="scatter",
    )(xt, ys)


def gather_actions(j, c, at, full, send_sem, recv_sem):
    first, rows = colour(j, c)
    axes = ORDERS[j][c]
    names = []
    for phase in (2, 1, 0):
        for s in range(1, SIZES[axes[phase]] // 2 + 1):
            names.append((phase, s))

    def copy(number, d):
        phase, s = names[number]
        axis = axes[phase]
        h = SIZES[axis] // 2
        sign = (1, -1)[d]
        index = {a: at[a] for a in axes[:phase]}
        index[axis] = shifted(at, axis, -(s - 1) * sign)
        place = (j, slice(None), *place_of(index, d if s == h else None, first, rows))
        return pltpu.make_async_remote_copy(
            src_ref=full.at[place],
            dst_ref=full.at[place],
            send_sem=send_sem.at[j, c, d],
            recv_sem=recv_sem.at[j, c, number, d],
            device_id=device(at, axis, shifted(at, axis, sign)),
            device_id_type=MESH,
        )

    def arriving(number, d):
        phase, s = names[number]
        axis = axes[phase]
        h = SIZES[axis] // 2
        sign = (1, -1)[d]
        index = {a: at[a] for a in axes[:phase]}
        index[axis] = shifted(at, axis, -s * sign)
        place = (j, slice(None), *place_of(index, d if s == h else None, first, rows))
        return pltpu.make_async_remote_copy(
            src_ref=full.at[place],
            dst_ref=full.at[place],
            send_sem=send_sem.at[j, c, d],
            recv_sem=recv_sem.at[j, c, number, d],
            device_id=device(at, axis, shifted(at, axis, sign)),
            device_id_type=MESH,
        )

    def action(number):
        def run():
            if number > 0:
                for d in range(2):
                    arriving(number - 1, d).wait_recv()
                for d in range(2):
                    copy(number - 1, d).wait_send()
            if number < len(names):
                for d in range(2):
                    copy(number, d).start()

        return run

    return [action(n) for n in range(len(names) + 1)]


def sum_actions(at, squares_ref, total_ref, boxes, send_sem, recv_sem):
    order = ("z", "x", "y")

    def copies(n):
        axis = order[n]
        base = sum(SIZES[a] - 1 for a in order[:n])
        box = boxes[axis]
        return [
            pltpu.make_async_remote_copy(
                src_ref=box.at[at[axis]],
                dst_ref=box.at[at[axis]],
                send_sem=send_sem.at[base + by - 1],
                recv_sem=recv_sem.at[base + by - 1],
                device_id=device(at, axis, shifted(at, axis, by)),
                device_id_type=MESH,
            )
            for by in range(1, SIZES[axis])
        ]

    def action(n):
        def run():
            if n == 0:
                value = squares_ref[...]
            else:
                for one in copies(n - 1):
                    one.wait()
                box = boxes[order[n - 1]]
                value = box[0]
                for i in range(1, SIZES[order[n - 1]]):
                    value = value + box[i]
            if n == len(order):
                total_ref[...] = value
                return
            boxes[order[n]][at[order[n]]] = value
            for one in copies(n):
                one.start()

        return run

    return [action(n) for n in range(len(order) + 1)]


def gather_kernel(shard_ref, squares_ref, out_ref, total_ref, full, box_x, box_y, box_z, load_sem, out_sem, send_sem, recv_sem, sum_send, sum_recv):
    at = here()
    mine = full.at[:, :, at["x"], at["y"], at["z"]]
    load = pltpu.make_async_copy(shard_ref, mine, load_sem)
    load.start()
    meet(at)
    load.wait()
    sums = sum_actions(at, squares_ref, total_ref, {"x": box_x, "y": box_y, "z": box_z}, sum_send, sum_recv)
    sums[0]()
    streams = {(j, c): gather_steps(j, c) for j in range(3) for c in range(3)}
    events = gather_order(streams)
    actions = {(j, c): gather_actions(j, c, at, full, send_sem, recv_sem) for j, c in streams}
    count = dict.fromkeys(streams, 0)
    left = {j: 3 for j in range(3)}
    outs = [pltpu.make_async_copy(full.at[j], out_ref.at[j], out_sem.at[j]) for j in range(3)]
    summed = 1
    for t, key in events:
        while summed < len(sums) and t > 5.0 * summed:
            sums[summed]()
            summed += 1
        actions[key][count[key]]()
        count[key] += 1
        if count[key] == len(actions[key]):
            left[key[0]] -= 1
            if left[key[0]] == 0:
                outs[key[0]].start()
    for one in outs:
        one.wait()


def gathered(shards, squares):
    sent = 6 * D * FF * 2
    return pl.pallas_call(
        gather_kernel,
        out_shape=(jax.ShapeDtypeStruct((3, 2, 4, 4, 8, SHARD, LANES), BF), jax.ShapeDtypeStruct((8, LANES), F32)),
        in_specs=[pl.BlockSpec(memory_space=pltpu.HBM), pl.BlockSpec(memory_space=pltpu.VMEM)],
        out_specs=[pl.BlockSpec(memory_space=pltpu.HBM), pl.BlockSpec(memory_space=pltpu.VMEM)],
        scratch_shapes=[
            pltpu.VMEM((3, 2, 4, 4, 8, SHARD, LANES), BF),
            pltpu.VMEM((4, 8, LANES), F32),
            pltpu.VMEM((4, 8, LANES), F32),
            pltpu.VMEM((8, 8, LANES), F32),
            pltpu.SemaphoreType.DMA,
            pltpu.SemaphoreType.DMA((3,)),
            pltpu.SemaphoreType.DMA((3, 3, 2)),
            pltpu.SemaphoreType.DMA((3, 3, 8, 2)),
            pltpu.SemaphoreType.DMA((13,)),
            pltpu.SemaphoreType.DMA((13,)),
        ],
        compiler_params=pltpu.CompilerParams(collective_id=1, has_side_effects=True, vmem_limit_bytes=LIMIT),
        cost_estimate=pl.CostEstimate(flops=sent * 100, bytes_accessed=2 * sent, transcendentals=0),
        name="gather",
    )(shards, squares)


def adamw_kernel(total_ref, g_ref, *refs):
    ins, outs, factor_ref = refs[:9], refs[9:18], refs[18]

    @pl.when(jnp.logical_and(pl.program_id(0) == 0, pl.program_id(1) == 0))
    def _():
        mean = jnp.sum(total_ref[...], keepdims=True) * (1.0 / (6 * D * FF))
        factor_ref[...] = jnp.broadcast_to(jnp.minimum(1.0, 0.5 * lax.rsqrt(mean + 1e-30)), factor_ref.shape)

    factor = factor_ref[0:1, :]

    def one(j, g, place):
        w_ref, m_ref, v_ref = ins[3 * j : 3 * j + 3]
        wo_ref, mo_ref, vo_ref = outs[3 * j : 3 * j + 3]
        w = w_ref[place].astype(F32)
        m = 0.9 * m_ref[place] + 0.1 * g
        v = 0.95 * v_ref[place] + 0.05 * g * g
        step = m * lax.rsqrt(v + 1e-8) + 0.1 * w
        wo_ref[place] = (w - 0.02 * step).astype(BF)
        mo_ref[place] = m
        vo_ref[place] = v

    for half in range(PANEL // LANES):
        lanes = pl.ds(half * LANES, LANES)

        def body(i, carry):
            here_rows = pl.ds(pl.multiple_of(half * D + i * 128, 128), 128)
            rows = pl.ds(pl.multiple_of(i * 128, 128), 128)
            for j in (1, 2):
                one(j, g_ref[j, here_rows, :].astype(F32) * factor, (rows, lanes))
            return carry

        lax.fori_loop(0, D // 128, body, 0)
        for i in range(D // 128):
            g = g_ref[0, pl.ds(half * D + i * 128, 128), :].astype(F32) * factor
            one(0, g.T, (lanes, pl.ds(i * 128, 128)))


def adamw(total, g, weights):
    wide = pl.BlockSpec((None, D, PANEL), lambda l, p: (l, 0, p))
    tall = pl.BlockSpec((None, PANEL, D), lambda l, p: (l, p, 0))
    specs = [tall] * 3 + [wide] * 6
    arrays = [a for one in weights for a in one]
    return pl.pallas_call(
        adamw_kernel,
        grid=(2, PANELS),
        out_shape=[jax.ShapeDtypeStruct(a.shape, a.dtype) for a in arrays],
        in_specs=[
            pl.BlockSpec((8, LANES), lambda l, p: (0, 0)),
            pl.BlockSpec((3, None, PANEL // LANES * D, LANES), lambda l, p: (0, 1 - l, p, 0)),
            *specs,
        ],
        out_specs=specs,
        scratch_shapes=[pltpu.VMEM((8, LANES), F32)],
        compiler_params=pltpu.CompilerParams(vmem_limit_bytes=LIMIT, dimension_semantics=("arbitrary", "arbitrary")),
        cost_estimate=pl.CostEstimate(flops=6 * D * FF * 30, bytes_accessed=6 * D * FF * 22, transcendentals=6 * D * FF),
        name="adamw",
    )(total, g, *arrays)


def solution(mesh):
    def step(x, dy, w_gate, w_up, w_down, m_gate, m_up, m_down, v_gate, v_up, v_down):
        xt, ys = row_wise(x[0], dy[0], w_gate, w_up, w_down)
        shards, squares = scattered(xt, ys)
        full, total = gathered(shards, squares)
        new = adamw(
            total,
            full.reshape(3, 2, 128 * SHARD, LANES),
            ((w_down, m_down, v_down), (w_gate, m_gate, v_gate), (w_up, m_up, v_up)),
        )
        return tuple(new[3 * j + which] for which in range(3) for j in (1, 2, 0))

    return jax.shard_map(
        step,
        mesh=mesh,
        in_specs=(P(("rep", "dp"), None, None),) * 2 + (P(None, None, None),) * 9,
        out_specs=(P("rep", None, None),) * 9,
        check_vma=False,
    )
```

```python
import functools

import jax
import jax.numpy as jnp
from jax import lax
from jax.experimental import pallas as pl
from jax.experimental.pallas import tpu as pltpu
from jax.sharding import PartitionSpec as P

BF, F32 = jnp.bfloat16, jnp.float32
MESH = pl.DeviceIdType.MESH
SIZES = {"x": 4, "y": 4, "z": 8}
AXES = ("x", "y", "z")
LANES = 128
SHARD = 128
D, FF, TOKENS = 896, 2304, 2048
PANEL = 256
PANELS = FF // PANEL
LIMIT = 66_900_000
ORDERS = tuple((("z", *second), ("x", "y", "z"), ("y", "x", "z")) for second in (("x", "y"), ("y", "x"), ("x", "y")))
ROWS = ((48, 48, 32), (48, 32, 48), (32, 48, 48))


def colour(j, c):
    return sum(ROWS[j][:c]), ROWS[j][c]


def here():
    d = lax.axis_index("dp")
    return {"x": d // 32, "y": (d // 8) % 4, "z": d % 8}


def device(at, axis, value):
    at = dict(at, **{axis: value})
    return {"dp": (at["x"] * 4 + at["y"]) * 8 + at["z"]}


def shifted(at, axis, by):
    n = SIZES[axis]
    return (at[axis] + (by % n)) % n


def meet(at):
    barrier = pltpu.get_barrier_semaphore()
    peers = [(axis, by) for axis in AXES for by in range(1, SIZES[axis])]
    for axis, by in peers:
        pl.semaphore_signal(barrier, inc=1, device_id=device(at, axis, shifted(at, axis, by)), device_id_type=MESH)
    pl.semaphore_wait(barrier, len(peers))


def place_of(fixed, half, first, rows):
    place, halved = [], half is None
    for a in AXES:
        if a in fixed:
            place.append(fixed[a])
        elif not halved:
            n = SIZES[a] // 2
            place.append(pl.ds(half * n, n))
            halved = True
        else:
            place.append(slice(None))
    begin, size = first, rows
    if not halved:
        one = (rows // 2 + 15) // 16 * 16
        begin, size = (first, one) if half == 0 else (first + one, rows - one)
    return tuple(place) + (pl.ds(begin, size), slice(None))


RATE, LATENCY, SERVE = 45.0e3, 2.2, 0.3


def bytes_of(j, c, phase, part):
    size = SHARD * SHARD * LANES * 2 * ROWS[j][c] // SHARD
    for axis in ORDERS[j][c][: phase + 1]:
        size //= SIZES[axis]
    return size * part


def gather_steps(j, c):
    out = []
    for phase, axis in reversed(list(enumerate(ORDERS[j][c]))):
        h = SIZES[axis] // 2
        for s in range(1, h + 1):
            out.append((axis, 2 * bytes_of(j, c, phase, 0.5 if s == h else 1)))
    return out


def gather_order(streams):
    free = dict.fromkeys(AXES, 0.0)
    arrival, position = {}, {}
    now, out = 0.0, []
    waiting = list(streams)

    def send(key, at):
        axis, size = streams[key][at]
        free[axis] = max(now, free[axis]) + size / RATE
        arrival[key], position[key] = free[axis] + LATENCY, at

    while waiting or arrival:
        choices = sorted((t, key) for key, t in arrival.items())
        start = next((key for key in waiting if free[streams[key][0][0]] < now + 3.0), None)
        if start is not None:
            now += SERVE
            out.append((now, start))
            waiting.remove(start)
            send(start, 0)
        elif choices and choices[0][0] <= now:
            key = choices[0][1]
            now += SERVE
            out.append((now, key))
            del arrival[key]
            if position[key] + 1 < len(streams[key]):
                send(key, position[key] + 1)
        else:
            later = [choices[0][0]] if choices else []
            later += [free[streams[key][0][0]] - 3.0 for key in waiting]
            now = max(now + 0.01, min(later))
    return out


TB = 512


def dot(a, b):
    return lax.dot_general(a, b, (((1,), (0,)), ((), ())), preferred_element_type=F32)


def dot_t(a, b):
    return lax.dot_general(a, b, (((1,), (1,)), ((), ())), preferred_element_type=F32)


def rows_kernel(x_ref, dy_ref, wg_ref, wu_ref, wd_ref, xt_hbm, ys_hbm, wg, wu, wd, gate0, up0, a_buf, h_buf, xt_ref, ys_ref, load_sem, xt_sem, ys_sem, late_sem):
    block = pl.program_id(0)
    first, last = block == 0, block == pl.num_programs(0) - 1
    loads = {
        (name, layer): pltpu.make_async_copy(ref.at[layer], buf.at[layer], load_sem.at[n, layer])
        for n, (name, ref, buf) in enumerate((("g", wg_ref, wg), ("u", wu_ref, wu), ("d", wd_ref, wd)))
        for layer in range(2)
    }

    @pl.when(first)
    def _():
        for layer in range(2):
            for name in "gud":
                loads[name, layer].start()

    def need(*which):
        @pl.when(first)
        def _():
            for one in which:
                loads[one].wait()

    tokens = pl.ds(pl.multiple_of(block * TB, TB), TB)

    def xt_out(*at):
        return pltpu.make_async_copy(xt_ref.at[at], xt_hbm.at[(*at, slice(None), tokens)], xt_sem.at[at])

    def ys_out(*at):
        return pltpu.make_async_copy(ys_ref.at[at], ys_hbm.at[(*at, tokens, slice(None))], ys_sem.at[at])

    def late_out(j, third):
        lanes = pl.ds(third * 3 * PANEL, 3 * PANEL)
        return pltpu.make_async_copy(ys_ref.at[1, j, :, lanes], ys_hbm.at[1, j, tokens, lanes], late_sem.at[j - 1, third])

    late_outs = [late_out(j, third) for j in (1, 2) for third in range(3)]

    def free(*outs):
        @pl.when(jnp.logical_not(first))
        def _():
            for one in outs:
                one.wait()

    def scale_of(wide):
        return lax.rsqrt(jnp.mean(wide * wide, -1, keepdims=True) + 1e-6)

    x = x_ref[...].astype(F32)
    a0 = (x * scale_of(x)).astype(BF)
    a_buf[...] = a0
    free(xt_out(1, 1), xt_out(0, 0))
    xt_ref[1, 1] = a0.T
    xt_ref[0, 0] = dy_ref[...].T
    xt_out(1, 1).start()
    xt_out(0, 0).start()
    free(ys_out(1, 0))
    need(("g", 0), ("u", 0))

    def panels(body):
        for p in range(PANELS):
            body(p)

    def at(p):
        return pl.ds(p * PANEL, PANEL)

    def forward0(p):
        gate, up = dot(a_buf[...], wg[0, :, at(p)]), dot(a_buf[...], wu[0, :, at(p)])
        gate0[:, at(p)], up0[:, at(p)] = gate, up
        ys_ref[1, 0, :, at(p)] = (gate * lax.logistic(gate) * up).astype(BF)

    panels(forward0)
    ys_out(1, 0).start()
    need(("d", 0))
    h = x + dot(ys_ref[1, 0], wd[0]).astype(BF).astype(F32)
    h = h.astype(BF).astype(F32)
    h_buf[...] = h
    a1 = (h * scale_of(h)).astype(BF)
    a_buf[...] = a1
    free(xt_out(0, 1))
    xt_ref[0, 1] = a1.T
    xt_out(0, 1).start()
    free(ys_out(0, 0), ys_out(0, 1), ys_out(0, 2))
    need(("g", 1), ("u", 1), ("d", 1))

    def back(d, gate, up):
        d = d.astype(BF).astype(F32)
        s = lax.logistic(gate)
        silu = gate * s
        return (d * up * (s + silu * (1.0 - s))).astype(BF), (d * silu).astype(BF), (silu * up).astype(BF)

    def both1(p):
        gate, up = dot(a_buf[...], wg[1, :, at(p)]), dot(a_buf[...], wu[1, :, at(p)])
        d = dot_t(dy_ref[...], wd[1, at(p), :])
        ys_ref[0, 1, :, at(p)], ys_ref[0, 2, :, at(p)], ys_ref[0, 0, :, at(p)] = back(d, gate, up)

    panels(both1)
    for j in range(3):
        ys_out(0, j).start()
    da = dot_t(ys_ref[0, 1], wg[1]).astype(BF).astype(F32) + dot_t(ys_ref[0, 2], wu[1]).astype(BF).astype(F32)
    da = da.astype(BF).astype(F32)
    h = h_buf[...]
    scale = scale_of(h)
    dh = scale * da - h * (scale * scale * scale * jnp.mean(da * h, -1, keepdims=True))
    dh = (dy_ref[...].astype(F32) + dh.astype(BF).astype(F32)).astype(BF)
    a_buf[...] = dh
    free(xt_out(1, 0), *late_outs)
    xt_ref[1, 0] = dh.T
    xt_out(1, 0).start()

    def back0(p):
        d = dot_t(a_buf[...], wd[0, at(p), :])
        ys_ref[1, 1, :, at(p)], ys_ref[1, 2, :, at(p)], _ = back(d, gate0[:, at(p)], up0[:, at(p)])

    for p in range(PANELS):
        back0(p)
        if (p + 1) % 3 == 0:
            for j in (1, 2):
                late_out(j, p // 3).start()

    @pl.when(last)
    def _():
        for g in range(2):
            for kind in range(2):
                xt_out(g, kind).wait()
        for one in (ys_out(0, 0), ys_out(0, 1), ys_out(0, 2), ys_out(1, 0), *late_outs):
            one.wait()


def row_wise(x, dy, w_gate, w_up, w_down):
    tokens = x.shape[0]
    return pl.pallas_call(
        rows_kernel,
        grid=(tokens // TB,),
        out_shape=(jax.ShapeDtypeStruct((2, 2, D, tokens), BF), jax.ShapeDtypeStruct((2, 3, tokens, FF), BF)),
        in_specs=[pl.BlockSpec((TB, D), lambda i: (i, 0))] * 2 + [pl.BlockSpec(memory_space=pltpu.HBM)] * 3,
        out_specs=[pl.BlockSpec(memory_space=pltpu.HBM)] * 2,
        scratch_shapes=[
            pltpu.VMEM((2, D, FF), BF),
            pltpu.VMEM((2, D, FF), BF),
            pltpu.VMEM((2, FF, D), BF),
            pltpu.VMEM((TB, FF), F32),
            pltpu.VMEM((TB, FF), F32),
            pltpu.VMEM((TB, D), BF),
            pltpu.VMEM((TB, D), F32),
            pltpu.VMEM((2, 2, D, TB), BF),
            pltpu.VMEM((2, 3, TB, FF), BF),
            pltpu.SemaphoreType.DMA((3, 2)),
            pltpu.SemaphoreType.DMA((2, 2)),
            pltpu.SemaphoreType.DMA((2, 3)),
            pltpu.SemaphoreType.DMA((2, 3)),
        ],
        compiler_params=pltpu.CompilerParams(vmem_limit_bytes=LIMIT, dimension_semantics=("arbitrary",)),
        cost_estimate=pl.CostEstimate(flops=9 * 2 * tokens * D * FF, bytes_accessed=100_000_000, transcendentals=0),
        name="rows",
    )(x, dy, w_gate, w_up, w_down)


def scatter_actions(j, c, at, own, recv, send_sem, recv_sem, finish):
    first, rows = colour(j, c)
    axes = ORDERS[j][c]

    def add(target, buffers):
        def body(i, carry):
            place = (...,) if i is None else (i,)
            value = target[place].astype(F32)
            for b in buffers:
                value = value + b[place].astype(F32)
            target[place] = value.astype(BF)
            return carry

        if len(target.shape) == 4:
            lax.fori_loop(0, target.shape[0], body, 0)
        else:
            body(None, 0)

    def parts(phase):
        axis = axes[phase]
        h = SIZES[axis] // 2
        fixed = {a: at[a] for a in axes[:phase]}
        buffer = recv[(j * 3 + c) * 3 + phase]
        base = sum(SIZES[a] // 2 for a in axes[:phase])

        def owner(by):
            return dict(fixed, **{axis: shifted(at, axis, by)})

        def slot(s, d):
            index = owner(0)
            if s > 1:
                return (2 * s - 3 + d,)
            place = place_of(index, d, 0, rows)
            return (0,) + tuple(one for a, one in zip(AXES, place[:3], strict=True) if a not in index) + place[3:]

        def copy(g, s, d):
            sign = (1, -1)[d]
            return pltpu.make_async_remote_copy(
                src_ref=own.at[(g, j, *place_of(owner((h - s + 1) * sign), d if s == 1 else None, first, rows))],
                dst_ref=buffer.at[(g, *slot(s, d))],
                send_sem=send_sem.at[g, j, c, d],
                recv_sem=recv_sem.at[g, j, c, base + s - 1, d],
                device_id=device(at, axis, shifted(at, axis, sign)),
                device_id_type=MESH,
            )

        def step(g, s):
            for d in range(2):
                copy(g, s, d).wait_recv()
            if s < h:
                for d in range(2):
                    by = (h - s) * (1, -1)[d]
                    place = place_of(owner(by), d if s == 1 else None, first, rows)
                    add(own.at[(g, j, *place)], [buffer.at[(g, *slot(s, d))]])
            else:
                place = place_of(owner(0), None, first, rows)
                add(own.at[(g, j, *place)], [buffer.at[(g, *slot(s, d))] for d in range(2)])

        return h, copy, step

    def action(number):
        def run(g):
            left, phase = number, 0
            while phase < 3 and left > SIZES[axes[phase]] // 2:
                left -= SIZES[axes[phase]] // 2
                phase += 1
            h, copy, step = parts(phase)
            if left > 0:
                step(g, left)
            before = [copy(g, left, d) for d in range(2)] if left > 0 else []
            if left == h:
                if phase == 2:
                    for one in before:
                        one.wait_send()
                    finish(g, j, c, own.at[(g, j, *place_of(at, None, first, rows))])
                    return
                _, copy, _ = parts(phase + 1)
                left = 0
            for one in before:
                one.wait_send()
            for d in range(2):
                copy(g, left + 1, d).start()

        return run

    return [action(n) for n in range(1 + sum(SIZES[a] // 2 for a in axes))]


SLOTS = (
    ((2, 7, 5), (2, 8, 5), (2, 1, 6), (2, 4, 6), (1, 7, 1), (1, 3, 2),),
    ((1, 6, 2), (1, 8, 1), (1, 4, 2), (2, 5, 6),),
    ((0, 2, 0), (0, 1, 0), (0, 0, 0), (1, 0, 4), (2, 0, 6),),
    ((2, 2, 6), (1, 3, 3), (2, 6, 6),),
    ((1, 5, 2), (2, 7, 6), (1, 2, 3), (0, 0, 1), (1, 7, 2), (1, 1, 3), (2, 3, 6), (0, 1, 1),),
    ((0, 5, 0), (0, 3, 0), (0, 2, 1),),
    ((1, 6, 3), (1, 8, 2), (1, 5, 3), (0, 0, 2), (2, 8, 6), (1, 4, 3),),
    ((1, 7, 3), (2, 4, 7), (0, 4, 0),),
    ((1, 8, 3), (2, 1, 7), (2, 2, 7), (2, 5, 7), (2, 6, 7), (0, 8, 0), (1, 2, 4), (2, 0, 7), (1, 1, 4), (0, 6, 0), (1, 3, 4), (2, 7, 7), (1, 4, 4), (1, 6, 4), (1, 5, 4), (0, 7, 0), (2, 3, 7), (2, 8, 7), (0, 3, 1), (0, 5, 1), (2, 1, 8), (0, 1, 2), (2, 2, 8), (1, 0, 5), (1, 2, 5), (2, 5, 8), (1, 1, 5), (1, 7, 4), (1, 8, 4), (1, 4, 5), (2, 4, 8), (2, 0, 8), (1, 5, 5), (0, 4, 1), (2, 6, 8), (1, 6, 5), (0, 2, 2), (0, 6, 1), (1, 3, 5), (0, 0, 3), (2, 7, 8), (2, 3, 8), (2, 8, 8),),
    (),
)


def scatter_kernel(xt_ref, ys_ref, shard_ref, squares_ref, own, *refs):
    recv, refs = refs[:27], refs[27:]
    xbuf, ybuf, x_sem, y_sem, send_sem, recv_sem = refs
    at = here()
    total = PANELS

    def load_x(g, kind):
        return pltpu.make_async_copy(xt_ref.at[g, kind], xbuf.at[kind], x_sem.at[kind])

    def load_y(g, n):
        copies = []
        for q in range(3):
            lanes = pl.ds(pl.multiple_of((n % 3) * (3 * PANEL) + q * PANEL, PANEL), PANEL)
            copies.append(pltpu.make_async_copy(ys_ref.at[g, n // 3, :, lanes], ybuf.at[(g + n) % 2, q], y_sem.at[(g + n) % 2, q]))
        return copies

    load_x(0, 0).start()
    for one in load_y(0, 0):
        one.start()
    load_x(0, 1).start()
    squares_ref[...] = jnp.zeros_like(squares_ref)
    for g in range(2):
        for j in range(3):
            for z in (6, 7):
                own[g, j, 3, 3, z] = jnp.zeros((SHARD, LANES), BF)
    meet(at)

    def finish(g, j, c, region):
        first, rows = colour(j, c)
        value = region[...]
        shard_ref[j, g, pl.ds(first, rows), :] = value
        wide = value.astype(F32)
        squares_ref[...] += jnp.sum((wide * wide).reshape(rows // 8, 8, LANES), axis=0)

    actions = [scatter_actions(j, c, at, own, recv, send_sem, recv_sem, finish) for j in range(3) for c in range(3)]
    rounds = 2 + max(late for todo in SLOTS for late, _, _ in todo)

    def group(i, carry):
        def slot(n, carry):
            @pl.when(jnp.logical_and(n < total, i < 2))
            def _():
                j = n // 3
                kind = jnp.minimum(j, 1)

                @pl.when(n + 1 < total)
                def _():
                    for one in load_y(i, n + 1):
                        one.start()

                @pl.when(n == 0)
                def _():
                    load_x(i, 0).wait()

                @pl.when(n == 3)
                def _():
                    load_x(i, 1).wait()

                    @pl.when(i < 1)
                    def _():
                        load_x(i + 1, 0).start()

                for one in load_y(i, n):
                    one.wait()
                for q in range(3):
                    out = dot(xbuf[kind], ybuf[(i + n) % 2, q])
                    for half in range(PANEL // LANES):
                        for b in range(D // SHARD):
                            d = (2 * (3 * (n % 3) + q) + half) * (D // SHARD) + b
                            block = out[b * SHARD : (b + 1) * SHARD, half * LANES : (half + 1) * LANES]
                            own[i, j, d // 32, (d // 8) % 4, d % 8] = block.astype(BF)

                @pl.when(jnp.logical_and(n == total - 1, i < 1))
                def _():
                    load_x(i + 1, 1).start()
                    for one in load_y(i + 1, 0):
                        one.start()

            def serve(todo):
                for late, key, which in todo:
                    pl.when(jnp.logical_and(i >= late, i < 2 + late))(functools.partial(actions[key][which], i - late))

            for number, todo in enumerate(SLOTS):
                if todo:
                    pl.when(n == number)(functools.partial(serve, todo))
            return carry

        lax.fori_loop(0, total + 1, slot, 0)
        return carry

    lax.fori_loop(0, rounds, group, 0)


def recv_shapes():
    shapes = []
    for j in range(3):
        for c in range(3):
            for phase in range(3):
                axes = ORDERS[j][c]
                left = tuple(SIZES[a] for a in AXES if a not in axes[: phase + 1])
                shapes.append(pltpu.VMEM((2, SIZES[axes[phase]] - 1, *left, ROWS[j][c], LANES), BF))
    return shapes


def scattered(xt, ys):
    sent = 6 * D * FF * 2
    return pl.pallas_call(
        scatter_kernel,
        out_shape=(jax.ShapeDtypeStruct((3, 2, SHARD, LANES), BF), jax.ShapeDtypeStruct((8, LANES), F32)),
        in_specs=[pl.BlockSpec(memory_space=pltpu.HBM)] * 2,
        out_specs=[pl.BlockSpec(memory_space=pltpu.VMEM)] * 2,
        scratch_shapes=[
            pltpu.VMEM((2, 3, 4, 4, 8, SHARD, LANES), BF),
            *recv_shapes(),
            pltpu.VMEM((2, D, TOKENS), BF),
            pltpu.VMEM((2, 3, TOKENS, PANEL), BF),
            pltpu.SemaphoreType.DMA((2,)),
            pltpu.SemaphoreType.DMA((2, 3)),
            pltpu.SemaphoreType.DMA((2, 3, 3, 2)),
            pltpu.SemaphoreType.DMA((2, 3, 3, 8, 2)),
        ],
        compiler_params=pltpu.CompilerParams(collective_id=0, has_side_effects=True, vmem_limit_bytes=LIMIT),
        cost_estimate=pl.CostEstimate(flops=6 * 2 * TOKENS * D * FF, bytes_accessed=3 * sent, transcendentals=0),
        name="scatter",
    )(xt, ys)


def gather_actions(j, c, at, full, send_sem, recv_sem):
    first, rows = colour(j, c)
    axes = ORDERS[j][c]
    names = []
    for phase in (2, 1, 0):
        for s in range(1, SIZES[axes[phase]] // 2 + 1):
            names.append((phase, s))

    def copy(number, d):
        phase, s = names[number]
        axis = axes[phase]
        h = SIZES[axis] // 2
        sign = (1, -1)[d]
        index = {a: at[a] for a in axes[:phase]}
        index[axis] = shifted(at, axis, -(s - 1) * sign)
        place = (j, slice(None), *place_of(index, d if s == h else None, first, rows))
        return pltpu.make_async_remote_copy(
            src_ref=full.at[place],
            dst_ref=full.at[place],
            send_sem=send_sem.at[j, c, d],
            recv_sem=recv_sem.at[j, c, number, d],
            device_id=device(at, axis, shifted(at, axis, sign)),
            device_id_type=MESH,
        )

    def arriving(number, d):
        phase, s = names[number]
        axis = axes[phase]
        h = SIZES[axis] // 2
        sign = (1, -1)[d]
        index = {a: at[a] for a in axes[:phase]}
        index[axis] = shifted(at, axis, -s * sign)
        place = (j, slice(None), *place_of(index, d if s == h else None, first, rows))
        return pltpu.make_async_remote_copy(
            src_ref=full.at[place],
            dst_ref=full.at[place],
            send_sem=send_sem.at[j, c, d],
            recv_sem=recv_sem.at[j, c, number, d],
            device_id=device(at, axis, shifted(at, axis, sign)),
            device_id_type=MESH,
        )

    def action(number):
        def run():
            if number > 0:
                for d in range(2):
                    arriving(number - 1, d).wait_recv()
                for d in range(2):
                    copy(number - 1, d).wait_send()
            if number < len(names):
                for d in range(2):
                    copy(number, d).start()

        return run

    return [action(n) for n in range(len(names) + 1)]


def sum_actions(at, squares_ref, total_ref, boxes, send_sem, recv_sem):
    order = ("z", "x", "y")

    def copies(n):
        axis = order[n]
        base = sum(SIZES[a] - 1 for a in order[:n])
        box = boxes[axis]
        return [
            pltpu.make_async_remote_copy(
                src_ref=box.at[at[axis]],
                dst_ref=box.at[at[axis]],
                send_sem=send_sem.at[base + by - 1],
                recv_sem=recv_sem.at[base + by - 1],
                device_id=device(at, axis, shifted(at, axis, by)),
                device_id_type=MESH,
            )
            for by in range(1, SIZES[axis])
        ]

    def action(n):
        def run():
            if n == 0:
                value = squares_ref[...]
            else:
                for one in copies(n - 1):
                    one.wait()
                box = boxes[order[n - 1]]
                value = box[0]
                for i in range(1, SIZES[order[n - 1]]):
                    value = value + box[i]
            if n == len(order):
                total_ref[...] = value
                return
            boxes[order[n]][at[order[n]]] = value
            for one in copies(n):
                one.start()

        return run

    return [action(n) for n in range(len(order) + 1)]


def gather_kernel(shard_ref, squares_ref, out_ref, total_ref, full, box_x, box_y, box_z, load_sem, out_sem, send_sem, recv_sem, sum_send, sum_recv):
    at = here()
    mine = full.at[:, :, at["x"], at["y"], at["z"]]
    load = pltpu.make_async_copy(shard_ref, mine, load_sem)
    load.start()
    meet(at)
    load.wait()
    sums = sum_actions(at, squares_ref, total_ref, {"x": box_x, "y": box_y, "z": box_z}, sum_send, sum_recv)
    sums[0]()
    streams = {(j, c): gather_steps(j, c) for j in range(3) for c in range(3)}
    events = gather_order(streams)
    actions = {(j, c): gather_actions(j, c, at, full, send_sem, recv_sem) for j, c in streams}
    count = dict.fromkeys(streams, 0)
    outs = {}
    for j, c in streams:
        place = (j, slice(None), *place_of({}, None, *colour(j, c)))
        outs[j, c] = pltpu.make_async_copy(full.at[place], out_ref.at[place], out_sem.at[j, c])
    summed = 1
    for t, key in events:
        while summed < len(sums) and t > 5.0 * summed:
            sums[summed]()
            summed += 1
        actions[key][count[key]]()
        count[key] += 1
        if count[key] == len(actions[key]):
            outs[key].start()
    for one in outs.values():
        one.wait()


def gathered(shards, squares):
    sent = 6 * D * FF * 2
    return pl.pallas_call(
        gather_kernel,
        out_shape=(jax.ShapeDtypeStruct((3, 2, 4, 4, 8, SHARD, LANES), BF), jax.ShapeDtypeStruct((8, LANES), F32)),
        in_specs=[pl.BlockSpec(memory_space=pltpu.HBM), pl.BlockSpec(memory_space=pltpu.VMEM)],
        out_specs=[pl.BlockSpec(memory_space=pltpu.HBM), pl.BlockSpec(memory_space=pltpu.VMEM)],
        scratch_shapes=[
            pltpu.VMEM((3, 2, 4, 4, 8, SHARD, LANES), BF),
            pltpu.VMEM((4, 8, LANES), F32),
            pltpu.VMEM((4, 8, LANES), F32),
            pltpu.VMEM((8, 8, LANES), F32),
            pltpu.SemaphoreType.DMA,
            pltpu.SemaphoreType.DMA((3, 3)),
            pltpu.SemaphoreType.DMA((3, 3, 2)),
            pltpu.SemaphoreType.DMA((3, 3, 8, 2)),
            pltpu.SemaphoreType.DMA((13,)),
            pltpu.SemaphoreType.DMA((13,)),
        ],
        compiler_params=pltpu.CompilerParams(collective_id=1, has_side_effects=True, vmem_limit_bytes=LIMIT),
        cost_estimate=pl.CostEstimate(flops=sent * 100, bytes_accessed=2 * sent, transcendentals=0),
        name="gather",
    )(shards, squares)


HALF = D // 2


def adamw_kernel(total_ref, down_g, gate_g0, gate_g1, up_g0, up_g1, *refs):
    ins, outs, factor_ref = refs[:9], refs[9:18], refs[18]

    @pl.when(pl.program_id(0) + pl.program_id(1) + pl.program_id(2) == 0)
    def _():
        mean = jnp.sum(total_ref[...], keepdims=True) * (1.0 / (6 * D * FF))
        factor_ref[...] = jnp.broadcast_to(jnp.minimum(1.0, 0.5 * lax.rsqrt(mean + 1e-30)), factor_ref.shape)

    factor = factor_ref[0:1, :]

    def one(j, g, place):
        w_ref, m_ref, v_ref = ins[3 * j : 3 * j + 3]
        wo_ref, mo_ref, vo_ref = outs[3 * j : 3 * j + 3]
        w = w_ref[place].astype(F32)
        m = 0.9 * m_ref[place] + 0.1 * g
        v = 0.95 * v_ref[place] + 0.05 * g * g
        step = m * lax.rsqrt(v + 1e-8) + 0.1 * w
        wo_ref[place] = (w - 0.02 * step).astype(BF)
        mo_ref[place] = m
        vo_ref[place] = v

    for half, gs in enumerate(((gate_g0, up_g0), (gate_g1, up_g1))):
        lanes = pl.ds(half * LANES, LANES)

        def body(i, carry):
            rows = pl.ds(pl.multiple_of(i * 64, 64), 64)
            for j, g_ref in zip((1, 2), gs, strict=True):
                one(j, g_ref[rows, :].astype(F32) * factor, (rows, lanes))
            return carry

        lax.fori_loop(0, HALF // 64, body, 0)
    for i in range(D // 128):
        g = down_g[pl.ds(i * 128, 128), :].astype(F32) * factor
        one(0, g.T, (slice(None), pl.ds(i * 128, 128)))


def adamw(total, g, weights):
    wide = pl.BlockSpec((None, HALF, PANEL), lambda l, p, r: (l, r, p))
    tall = pl.BlockSpec((None, LANES, D), lambda l, p, r: (l, 2 * p + r, 0))
    specs = [tall] * 3 + [wide] * 6
    arrays = [a for one in weights for a in one]

    def part(j, half):
        return pl.BlockSpec((None, None, HALF, LANES), lambda l, p, r: (j, 1 - l, 4 * p + 2 * half + r, 0))

    return pl.pallas_call(
        adamw_kernel,
        grid=(2, PANELS, 2),
        out_shape=[jax.ShapeDtypeStruct(a.shape, a.dtype) for a in arrays],
        in_specs=[
            pl.BlockSpec((8, LANES), lambda l, p, r: (0, 0)),
            pl.BlockSpec((None, None, D, LANES), lambda l, p, r: (0, 1 - l, 2 * p + r, 0)),
            part(1, 0),
            part(1, 1),
            part(2, 0),
            part(2, 1),
            *specs,
        ],
        out_specs=specs,
        scratch_shapes=[pltpu.VMEM((8, LANES), F32)],
        compiler_params=pltpu.CompilerParams(vmem_limit_bytes=LIMIT, dimension_semantics=("arbitrary",) * 3),
        cost_estimate=pl.CostEstimate(flops=6 * D * FF * 30, bytes_accessed=6 * D * FF * 22, transcendentals=6 * D * FF),
        name="adamw",
    )(total, g, g, g, g, g, *arrays)


def solution(mesh):
    def step(x, dy, w_gate, w_up, w_down, m_gate, m_up, m_down, v_gate, v_up, v_down):
        xt, ys = row_wise(x[0], dy[0], w_gate, w_up, w_down)
        shards, squares = scattered(xt, ys)
        full, total = gathered(shards, squares)
        new = adamw(
            total,
            full.reshape(3, 2, 128 * SHARD, LANES),
            ((w_down, m_down, v_down), (w_gate, m_gate, v_gate), (w_up, m_up, v_up)),
        )
        return tuple(new[3 * j + which] for which in range(3) for j in (1, 2, 0))

    return jax.shard_map(
        step,
        mesh=mesh,
        in_specs=(P(("rep", "dp"), None, None),) * 2 + (P(None, None, None),) * 9,
        out_specs=(P("rep", None, None),) * 9,
        check_vma=False,
    )
```

```python
import functools

import jax
import jax.numpy as jnp
from jax import lax
from jax.experimental import pallas as pl
from jax.experimental.pallas import tpu as pltpu
from jax.sharding import PartitionSpec as P

BF, F32 = jnp.bfloat16, jnp.float32
MESH = pl.DeviceIdType.MESH
SIZES = {"x": 4, "y": 4, "z": 8}
AXES = ("x", "y", "z")
LANES = 128
SHARD = 128
D, FF, TOKENS = 896, 2304, 2048
PANEL = 256
PANELS = FF // PANEL
LIMIT = 66_900_000
ORDERS = tuple((("z", *second), ("x", "y", "z"), ("y", "x", "z")) for second in (("x", "y"), ("y", "x"), ("x", "y")))
ROWS = ((48, 48, 32), (48, 32, 48), (32, 48, 48))


def colour(j, c):
    return sum(ROWS[j][:c]), ROWS[j][c]


def here():
    d = lax.axis_index("dp")
    return {"x": d // 32, "y": (d // 8) % 4, "z": d % 8}


def device(at, axis, value):
    at = dict(at, **{axis: value})
    return {"dp": (at["x"] * 4 + at["y"]) * 8 + at["z"]}


def shifted(at, axis, by):
    n = SIZES[axis]
    return (at[axis] + (by % n)) % n


def meet(at):
    barrier = pltpu.get_barrier_semaphore()
    peers = [(axis, by) for axis in AXES for by in range(1, SIZES[axis])]
    for axis, by in peers:
        pl.semaphore_signal(barrier, inc=1, device_id=device(at, axis, shifted(at, axis, by)), device_id_type=MESH)
    pl.semaphore_wait(barrier, len(peers))


def place_of(fixed, half, first, rows):
    place, halved = [], half is None
    for a in AXES:
        if a in fixed:
            place.append(fixed[a])
        elif not halved:
            n = SIZES[a] // 2
            place.append(pl.ds(half * n, n))
            halved = True
        else:
            place.append(slice(None))
    begin, size = first, rows
    if not halved:
        one = (rows // 2 + 15) // 16 * 16
        begin, size = (first, one) if half == 0 else (first + one, rows - one)
    return tuple(place) + (pl.ds(begin, size), slice(None))


RATE, LATENCY, SERVE = 45.0e3, 2.2, 0.3


def bytes_of(j, c, phase, part):
    size = SHARD * SHARD * LANES * 2 * ROWS[j][c] // SHARD
    for axis in ORDERS[j][c][: phase + 1]:
        size //= SIZES[axis]
    return size * part


def gather_steps(j, c):
    out = []
    for phase, axis in reversed(list(enumerate(ORDERS[j][c]))):
        h = SIZES[axis] // 2
        for s in range(1, h + 1):
            out.append((axis, 2 * bytes_of(j, c, phase, 0.5 if s == h else 1)))
    return out


def gather_order(streams):
    free = dict.fromkeys(AXES, 0.0)
    arrival, position = {}, {}
    now, out = 0.0, []
    waiting = list(streams)

    def send(key, at):
        axis, size = streams[key][at]
        free[axis] = max(now, free[axis]) + size / RATE
        arrival[key], position[key] = free[axis] + LATENCY, at

    while waiting or arrival:
        choices = sorted((t, key) for key, t in arrival.items())
        start = next((key for key in waiting if free[streams[key][0][0]] < now + 3.0), None)
        if start is not None:
            now += SERVE
            out.append((now, start))
            waiting.remove(start)
            send(start, 0)
        elif choices and choices[0][0] <= now:
            key = choices[0][1]
            now += SERVE
            out.append((now, key))
            del arrival[key]
            if position[key] + 1 < len(streams[key]):
                send(key, position[key] + 1)
        else:
            later = [choices[0][0]] if choices else []
            later += [free[streams[key][0][0]] - 3.0 for key in waiting]
            now = max(now + 0.01, min(later))
    return out


TB = 512


def dot(a, b):
    return lax.dot_general(a, b, (((1,), (0,)), ((), ())), preferred_element_type=F32)


def dot_t(a, b):
    return lax.dot_general(a, b, (((1,), (1,)), ((), ())), preferred_element_type=F32)


def rows_kernel(x_ref, dy_ref, wg_ref, wu_ref, wd_ref, xt_hbm, ys_hbm, wg, wu, wd, gate0, up0, a_buf, h_buf, xt_ref, ys_ref, load_sem, xt_sem, ys_sem, late_sem):
    block = pl.program_id(0)
    first, last = block == 0, block == pl.num_programs(0) - 1
    loads = {
        (name, layer): pltpu.make_async_copy(ref.at[layer], buf.at[layer], load_sem.at[n, layer])
        for n, (name, ref, buf) in enumerate((("g", wg_ref, wg), ("u", wu_ref, wu), ("d", wd_ref, wd)))
        for layer in range(2)
    }

    @pl.when(first)
    def _():
        for layer in range(2):
            for name in "gud":
                loads[name, layer].start()

    def need(*which):
        @pl.when(first)
        def _():
            for one in which:
                loads[one].wait()

    tokens = pl.ds(pl.multiple_of(block * TB, TB), TB)

    def xt_out(*at):
        return pltpu.make_async_copy(xt_ref.at[at], xt_hbm.at[(*at, slice(None), tokens)], xt_sem.at[at])

    def ys_out(*at):
        return pltpu.make_async_copy(ys_ref.at[at], ys_hbm.at[(*at, tokens, slice(None))], ys_sem.at[at])

    def late_out(j, third):
        lanes = pl.ds(third * 3 * PANEL, 3 * PANEL)
        return pltpu.make_async_copy(ys_ref.at[1, j, :, lanes], ys_hbm.at[1, j, tokens, lanes], late_sem.at[j - 1, third])

    late_outs = [late_out(j, third) for j in (1, 2) for third in range(3)]

    def free(*outs):
        @pl.when(jnp.logical_not(first))
        def _():
            for one in outs:
                one.wait()

    def scale_of(wide):
        return lax.rsqrt(jnp.mean(wide * wide, -1, keepdims=True) + 1e-6)

    x = x_ref[...].astype(F32)
    a0 = (x * scale_of(x)).astype(BF)
    a_buf[...] = a0
    free(xt_out(1, 1), xt_out(0, 0))
    xt_ref[1, 1] = a0.T
    xt_ref[0, 0] = dy_ref[...].T
    xt_out(1, 1).start()
    xt_out(0, 0).start()
    free(ys_out(1, 0))
    need(("g", 0), ("u", 0))

    def panels(body):
        for p in range(PANELS):
            body(p)

    def at(p):
        return pl.ds(p * PANEL, PANEL)

    def forward0(p):
        gate, up = dot(a_buf[...], wg[0, :, at(p)]), dot(a_buf[...], wu[0, :, at(p)])
        gate0[:, at(p)], up0[:, at(p)] = gate, up
        ys_ref[1, 0, :, at(p)] = (gate * lax.logistic(gate) * up).astype(BF)

    panels(forward0)
    ys_out(1, 0).start()
    need(("d", 0))
    h = x + dot(ys_ref[1, 0], wd[0]).astype(BF).astype(F32)
    h = h.astype(BF).astype(F32)
    h_buf[...] = h
    a1 = (h * scale_of(h)).astype(BF)
    a_buf[...] = a1
    free(xt_out(0, 1))
    xt_ref[0, 1] = a1.T
    xt_out(0, 1).start()
    free(ys_out(0, 0), ys_out(0, 1), ys_out(0, 2))
    need(("g", 1), ("u", 1), ("d", 1))

    def back(d, gate, up):
        d = d.astype(BF).astype(F32)
        s = lax.logistic(gate)
        silu = gate * s
        return (d * up * (s + silu * (1.0 - s))).astype(BF), (d * silu).astype(BF), (silu * up).astype(BF)

    def both1(p):
        gate, up = dot(a_buf[...], wg[1, :, at(p)]), dot(a_buf[...], wu[1, :, at(p)])
        d = dot_t(dy_ref[...], wd[1, at(p), :])
        ys_ref[0, 1, :, at(p)], ys_ref[0, 2, :, at(p)], ys_ref[0, 0, :, at(p)] = back(d, gate, up)

    panels(both1)
    for j in range(3):
        ys_out(0, j).start()
    da = dot_t(ys_ref[0, 1], wg[1]).astype(BF).astype(F32) + dot_t(ys_ref[0, 2], wu[1]).astype(BF).astype(F32)
    da = da.astype(BF).astype(F32)
    h = h_buf[...]
    scale = scale_of(h)
    dh = scale * da - h * (scale * scale * scale * jnp.mean(da * h, -1, keepdims=True))
    dh = (dy_ref[...].astype(F32) + dh.astype(BF).astype(F32)).astype(BF)
    a_buf[...] = dh
    free(xt_out(1, 0), *late_outs)
    xt_ref[1, 0] = dh.T
    xt_out(1, 0).start()

    def back0(p):
        d = dot_t(a_buf[...], wd[0, at(p), :])
        ys_ref[1, 1, :, at(p)], ys_ref[1, 2, :, at(p)], _ = back(d, gate0[:, at(p)], up0[:, at(p)])

    for p in range(PANELS):
        back0(p)
        if (p + 1) % 3 == 0:
            for j in (1, 2):
                late_out(j, p // 3).start()

    @pl.when(last)
    def _():
        for g in range(2):
            for kind in range(2):
                xt_out(g, kind).wait()
        for one in (ys_out(0, 0), ys_out(0, 1), ys_out(0, 2), ys_out(1, 0), *late_outs):
            one.wait()


def row_wise(x, dy, w_gate, w_up, w_down):
    tokens = x.shape[0]
    return pl.pallas_call(
        rows_kernel,
        grid=(tokens // TB,),
        out_shape=(jax.ShapeDtypeStruct((2, 2, D, tokens), BF), jax.ShapeDtypeStruct((2, 3, tokens, FF), BF)),
        in_specs=[pl.BlockSpec((TB, D), lambda i: (i, 0))] * 2 + [pl.BlockSpec(memory_space=pltpu.HBM)] * 3,
        out_specs=[pl.BlockSpec(memory_space=pltpu.HBM)] * 2,
        scratch_shapes=[
            pltpu.VMEM((2, D, FF), BF),
            pltpu.VMEM((2, D, FF), BF),
            pltpu.VMEM((2, FF, D), BF),
            pltpu.VMEM((TB, FF), F32),
            pltpu.VMEM((TB, FF), F32),
            pltpu.VMEM((TB, D), BF),
            pltpu.VMEM((TB, D), F32),
            pltpu.VMEM((2, 2, D, TB), BF),
            pltpu.VMEM((2, 3, TB, FF), BF),
            pltpu.SemaphoreType.DMA((3, 2)),
            pltpu.SemaphoreType.DMA((2, 2)),
            pltpu.SemaphoreType.DMA((2, 3)),
            pltpu.SemaphoreType.DMA((2, 3)),
        ],
        compiler_params=pltpu.CompilerParams(vmem_limit_bytes=LIMIT, dimension_semantics=("arbitrary",)),
        cost_estimate=pl.CostEstimate(flops=9 * 2 * tokens * D * FF, bytes_accessed=100_000_000, transcendentals=0),
        name="rows",
    )(x, dy, w_gate, w_up, w_down)


def scatter_actions(j, c, at, own, recv, send_sem, recv_sem, finish):
    first, rows = colour(j, c)
    axes = ORDERS[j][c]

    def add(target, buffers):
        def body(i, carry):
            place = (...,) if i is None else (i,)
            value = target[place].astype(F32)
            for b in buffers:
                value = value + b[place].astype(F32)
            target[place] = value.astype(BF)
            return carry

        if len(target.shape) == 4:
            lax.fori_loop(0, target.shape[0], body, 0)
        else:
            body(None, 0)

    def parts(phase):
        axis = axes[phase]
        h = SIZES[axis] // 2
        fixed = {a: at[a] for a in axes[:phase]}
        buffer = recv[(j * 3 + c) * 3 + phase]
        base = sum(SIZES[a] // 2 for a in axes[:phase])

        def owner(by):
            return dict(fixed, **{axis: shifted(at, axis, by)})

        def slot(s, d):
            index = owner(0)
            if s > 1:
                return (2 * s - 3 + d,)
            place = place_of(index, d, 0, rows)
            return (0,) + tuple(one for a, one in zip(AXES, place[:3], strict=True) if a not in index) + place[3:]

        def copy(g, s, d):
            sign = (1, -1)[d]
            return pltpu.make_async_remote_copy(
                src_ref=own.at[(g, j, *place_of(owner((h - s + 1) * sign), d if s == 1 else None, first, rows))],
                dst_ref=buffer.at[(g, *slot(s, d))],
                send_sem=send_sem.at[g, j, c, d],
                recv_sem=recv_sem.at[g, j, c, base + s - 1, d],
                device_id=device(at, axis, shifted(at, axis, sign)),
                device_id_type=MESH,
            )

        def step(g, s):
            for d in range(2):
                copy(g, s, d).wait_recv()
            if s < h:
                for d in range(2):
                    by = (h - s) * (1, -1)[d]
                    place = place_of(owner(by), d if s == 1 else None, first, rows)
                    add(own.at[(g, j, *place)], [buffer.at[(g, *slot(s, d))]])
            else:
                place = place_of(owner(0), None, first, rows)
                add(own.at[(g, j, *place)], [buffer.at[(g, *slot(s, d))] for d in range(2)])

        return h, copy, step

    def action(number):
        def run(g):
            left, phase = number, 0
            while phase < 3 and left > SIZES[axes[phase]] // 2:
                left -= SIZES[axes[phase]] // 2
                phase += 1
            h, copy, step = parts(phase)
            if left > 0:
                step(g, left)
            before = [copy(g, left, d) for d in range(2)] if left > 0 else []
            if left == h:
                if phase == 2:
                    for one in before:
                        one.wait_send()
                    finish(g, j, c, own.at[(g, j, *place_of(at, None, first, rows))])
                    return
                _, copy, _ = parts(phase + 1)
                left = 0
            for one in before:
                one.wait_send()
            for d in range(2):
                copy(g, left + 1, d).start()

        return run

    return [action(n) for n in range(1 + sum(SIZES[a] // 2 for a in axes))]


SLOTS = (
    ((2, 7, 5), (2, 8, 5), (2, 1, 6), (2, 4, 6), (1, 7, 1), (1, 3, 2),),
    ((1, 6, 2), (1, 8, 1), (1, 4, 2), (2, 5, 6),),
    ((0, 2, 0), (0, 1, 0), (0, 0, 0), (1, 0, 4), (2, 0, 6),),
    ((2, 2, 6), (1, 3, 3), (2, 6, 6),),
    ((1, 5, 2), (2, 7, 6), (1, 2, 3), (0, 0, 1), (1, 7, 2), (1, 1, 3), (2, 3, 6), (0, 1, 1),),
    ((0, 5, 0), (0, 3, 0), (0, 2, 1),),
    ((1, 6, 3), (1, 8, 2), (1, 5, 3), (0, 0, 2), (2, 8, 6), (1, 4, 3),),
    ((1, 7, 3), (2, 4, 7), (0, 4, 0),),
    ((1, 8, 3), (2, 1, 7), (2, 2, 7), (2, 5, 7), (2, 6, 7), (0, 8, 0), (1, 2, 4), (2, 0, 7), (1, 1, 4), (0, 6, 0), (1, 3, 4), (2, 7, 7), (1, 4, 4), (1, 6, 4), (1, 5, 4), (0, 7, 0), (2, 3, 7), (2, 8, 7), (0, 3, 1), (0, 5, 1), (2, 1, 8), (0, 1, 2), (2, 2, 8), (1, 0, 5), (1, 2, 5), (2, 5, 8), (1, 1, 5), (1, 7, 4), (1, 8, 4), (1, 4, 5), (2, 4, 8), (2, 0, 8), (1, 5, 5), (0, 4, 1), (2, 6, 8), (1, 6, 5), (0, 2, 2), (0, 6, 1), (1, 3, 5), (0, 0, 3), (2, 7, 8), (2, 3, 8), (2, 8, 8),),
    (),
)


def scatter_kernel(xt_ref, ys_ref, shard_ref, squares_ref, own, *refs):
    recv, refs = refs[:27], refs[27:]
    xbuf, ybuf, x_sem, y_sem, send_sem, recv_sem = refs
    at = here()
    total = PANELS

    def load_x(g, kind):
        return pltpu.make_async_copy(xt_ref.at[g, kind], xbuf.at[kind], x_sem.at[kind])

    def load_y(g, n):
        copies = []
        for q in range(3):
            lanes = pl.ds(pl.multiple_of((n % 3) * (3 * PANEL) + q * PANEL, PANEL), PANEL)
            copies.append(pltpu.make_async_copy(ys_ref.at[g, n // 3, :, lanes], ybuf.at[(g + n) % 2, q], y_sem.at[(g + n) % 2, q]))
        return copies

    load_x(0, 0).start()
    for one in load_y(0, 0):
        one.start()
    load_x(0, 1).start()
    squares_ref[...] = jnp.zeros_like(squares_ref)
    for g in range(2):
        for j in range(3):
            for z in (6, 7):
                own[g, j, 3, 3, z] = jnp.zeros((SHARD, LANES), BF)
    meet(at)

    def finish(g, j, c, region):
        first, rows = colour(j, c)
        value = region[...]
        shard_ref[j, g, pl.ds(first, rows), :] = value
        wide = value.astype(F32)
        squares_ref[...] += jnp.sum((wide * wide).reshape(rows // 8, 8, LANES), axis=0)

    actions = [scatter_actions(j, c, at, own, recv, send_sem, recv_sem, finish) for j in range(3) for c in range(3)]
    rounds = 2 + max(late for todo in SLOTS for late, _, _ in todo)

    def group(i, carry):
        def slot(n, carry):
            @pl.when(jnp.logical_and(n < total, i < 2))
            def _():
                j = n // 3
                kind = jnp.minimum(j, 1)

                @pl.when(n + 1 < total)
                def _():
                    for one in load_y(i, n + 1):
                        one.start()

                @pl.when(n == 0)
                def _():
                    load_x(i, 0).wait()

                @pl.when(n == 3)
                def _():
                    load_x(i, 1).wait()

                    @pl.when(i < 1)
                    def _():
                        load_x(i + 1, 0).start()

                for one in load_y(i, n):
                    one.wait()
                for q in range(3):
                    out = dot(xbuf[kind], ybuf[(i + n) % 2, q])
                    for half in range(PANEL // LANES):
                        for b in range(D // SHARD):
                            d = (2 * (3 * (n % 3) + q) + half) * (D // SHARD) + b
                            block = out[b * SHARD : (b + 1) * SHARD, half * LANES : (half + 1) * LANES]
                            own[i, j, d // 32, (d // 8) % 4, d % 8] = block.astype(BF)

                @pl.when(jnp.logical_and(n == total - 1, i < 1))
                def _():
                    load_x(i + 1, 1).start()
                    for one in load_y(i + 1, 0):
                        one.start()

            def serve(todo):
                for late, key, which in todo:
                    pl.when(jnp.logical_and(i >= late, i < 2 + late))(functools.partial(actions[key][which], i - late))

            for number, todo in enumerate(SLOTS):
                if todo:
                    pl.when(n == number)(functools.partial(serve, todo))
            return carry

        lax.fori_loop(0, total + 1, slot, 0)
        return carry

    lax.fori_loop(0, rounds, group, 0)


def recv_shapes():
    shapes = []
    for j in range(3):
        for c in range(3):
            for phase in range(3):
                axes = ORDERS[j][c]
                left = tuple(SIZES[a] for a in AXES if a not in axes[: phase + 1])
                shapes.append(pltpu.VMEM((2, SIZES[axes[phase]] - 1, *left, ROWS[j][c], LANES), BF))
    return shapes


def scattered(xt, ys):
    sent = 6 * D * FF * 2
    return pl.pallas_call(
        scatter_kernel,
        out_shape=(jax.ShapeDtypeStruct((3, 2, SHARD, LANES), BF), jax.ShapeDtypeStruct((8, LANES), F32)),
        in_specs=[pl.BlockSpec(memory_space=pltpu.HBM)] * 2,
        out_specs=[pl.BlockSpec(memory_space=pltpu.VMEM)] * 2,
        scratch_shapes=[
            pltpu.VMEM((2, 3, 4, 4, 8, SHARD, LANES), BF),
            *recv_shapes(),
            pltpu.VMEM((2, D, TOKENS), BF),
            pltpu.VMEM((2, 3, TOKENS, PANEL), BF),
            pltpu.SemaphoreType.DMA((2,)),
            pltpu.SemaphoreType.DMA((2, 3)),
            pltpu.SemaphoreType.DMA((2, 3, 3, 2)),
            pltpu.SemaphoreType.DMA((2, 3, 3, 8, 2)),
        ],
        compiler_params=pltpu.CompilerParams(collective_id=0, has_side_effects=True, vmem_limit_bytes=LIMIT),
        cost_estimate=pl.CostEstimate(flops=6 * 2 * TOKENS * D * FF, bytes_accessed=3 * sent, transcendentals=0),
        name="scatter",
    )(xt, ys)


def gather_actions(j, c, at, full, send_sem, recv_sem):
    first, rows = colour(j, c)
    axes = ORDERS[j][c]
    names = []
    for phase in (2, 1, 0):
        for s in range(1, SIZES[axes[phase]] // 2 + 1):
            names.append((phase, s))

    def copy(number, d):
        phase, s = names[number]
        axis = axes[phase]
        h = SIZES[axis] // 2
        sign = (1, -1)[d]
        index = {a: at[a] for a in axes[:phase]}
        index[axis] = shifted(at, axis, -(s - 1) * sign)
        place = (j, slice(None), *place_of(index, d if s == h else None, first, rows))
        return pltpu.make_async_remote_copy(
            src_ref=full.at[place],
            dst_ref=full.at[place],
            send_sem=send_sem.at[j, c, d],
            recv_sem=recv_sem.at[j, c, number, d],
            device_id=device(at, axis, shifted(at, axis, sign)),
            device_id_type=MESH,
        )

    def arriving(number, d):
        phase, s = names[number]
        axis = axes[phase]
        h = SIZES[axis] // 2
        sign = (1, -1)[d]
        index = {a: at[a] for a in axes[:phase]}
        index[axis] = shifted(at, axis, -s * sign)
        place = (j, slice(None), *place_of(index, d if s == h else None, first, rows))
        return pltpu.make_async_remote_copy(
            src_ref=full.at[place],
            dst_ref=full.at[place],
            send_sem=send_sem.at[j, c, d],
            recv_sem=recv_sem.at[j, c, number, d],
            device_id=device(at, axis, shifted(at, axis, sign)),
            device_id_type=MESH,
        )

    def action(number):
        def run():
            if number > 0:
                for d in range(2):
                    arriving(number - 1, d).wait_recv()
                for d in range(2):
                    copy(number - 1, d).wait_send()
            if number < len(names):
                for d in range(2):
                    copy(number, d).start()

        return run

    return [action(n) for n in range(len(names) + 1)]


def sum_actions(at, squares_ref, total_ref, boxes, send_sem, recv_sem):
    order = ("z", "x", "y")

    def copies(n):
        axis = order[n]
        base = sum(SIZES[a] - 1 for a in order[:n])
        box = boxes[axis]
        return [
            pltpu.make_async_remote_copy(
                src_ref=box.at[at[axis]],
                dst_ref=box.at[at[axis]],
                send_sem=send_sem.at[base + by - 1],
                recv_sem=recv_sem.at[base + by - 1],
                device_id=device(at, axis, shifted(at, axis, by)),
                device_id_type=MESH,
            )
            for by in range(1, SIZES[axis])
        ]

    def action(n):
        def run():
            if n == 0:
                value = squares_ref[...]
            else:
                for one in copies(n - 1):
                    one.wait()
                box = boxes[order[n - 1]]
                value = box[0]
                for i in range(1, SIZES[order[n - 1]]):
                    value = value + box[i]
            if n == len(order):
                total_ref[...] = value
                return
            boxes[order[n]][at[order[n]]] = value
            for one in copies(n):
                one.start()

        return run

    return [action(n) for n in range(len(order) + 1)]


def gather_kernel(shard_ref, squares_ref, out_ref, total_ref, full, box_x, box_y, box_z, load_sem, out_sem, send_sem, recv_sem, sum_send, sum_recv):
    at = here()
    mine = full.at[:, :, at["x"], at["y"], at["z"]]
    load = pltpu.make_async_copy(shard_ref, mine, load_sem)
    load.start()
    meet(at)
    load.wait()
    sums = sum_actions(at, squares_ref, total_ref, {"x": box_x, "y": box_y, "z": box_z}, sum_send, sum_recv)
    sums[0]()
    streams = {(j, c): gather_steps(j, c) for j in range(3) for c in range(3)}
    events = gather_order(streams)
    actions = {(j, c): gather_actions(j, c, at, full, send_sem, recv_sem) for j, c in streams}
    count = dict.fromkeys(streams, 0)
    outs = {}
    for j, c in streams:
        place = (j, slice(None), *place_of({}, None, *colour(j, c)))
        outs[j, c] = pltpu.make_async_copy(full.at[place], out_ref.at[place], out_sem.at[j, c])
    summed = 1
    for t, key in events:
        while summed < len(sums) and t > 5.0 * summed:
            sums[summed]()
            summed += 1
        actions[key][count[key]]()
        count[key] += 1
        if count[key] == len(actions[key]):
            outs[key].start()
    for one in outs.values():
        one.wait()


def gathered(shards, squares):
    sent = 6 * D * FF * 2
    return pl.pallas_call(
        gather_kernel,
        out_shape=(jax.ShapeDtypeStruct((3, 2, 4, 4, 8, SHARD, LANES), BF), jax.ShapeDtypeStruct((8, LANES), F32)),
        in_specs=[pl.BlockSpec(memory_space=pltpu.HBM), pl.BlockSpec(memory_space=pltpu.VMEM)],
        out_specs=[pl.BlockSpec(memory_space=pltpu.HBM), pl.BlockSpec(memory_space=pltpu.VMEM)],
        scratch_shapes=[
            pltpu.VMEM((3, 2, 4, 4, 8, SHARD, LANES), BF),
            pltpu.VMEM((4, 8, LANES), F32),
            pltpu.VMEM((4, 8, LANES), F32),
            pltpu.VMEM((8, 8, LANES), F32),
            pltpu.SemaphoreType.DMA,
            pltpu.SemaphoreType.DMA((3, 3)),
            pltpu.SemaphoreType.DMA((3, 3, 2)),
            pltpu.SemaphoreType.DMA((3, 3, 8, 2)),
            pltpu.SemaphoreType.DMA((13,)),
            pltpu.SemaphoreType.DMA((13,)),
        ],
        compiler_params=pltpu.CompilerParams(collective_id=1, has_side_effects=True, vmem_limit_bytes=LIMIT),
        cost_estimate=pl.CostEstimate(flops=sent * 100, bytes_accessed=2 * sent, transcendentals=0),
        name="gather",
    )(shards, squares)


def adamw_kernel(total_ref, g_ref, *refs):
    ins, outs, factor_ref = refs[:9], refs[9:18], refs[18]

    @pl.when(jnp.logical_and(pl.program_id(0) == 0, pl.program_id(1) == 0))
    def _():
        mean = jnp.sum(total_ref[...], keepdims=True) * (1.0 / (6 * D * FF))
        factor_ref[...] = jnp.broadcast_to(jnp.minimum(1.0, 0.5 * lax.rsqrt(mean + 1e-30)), factor_ref.shape)

    factor = factor_ref[0:1, :]

    def one(j, g, place):
        w_ref, m_ref, v_ref = ins[3 * j : 3 * j + 3]
        wo_ref, mo_ref, vo_ref = outs[3 * j : 3 * j + 3]
        w = w_ref[place].astype(F32)
        m = 0.9 * m_ref[place] + 0.1 * g
        v = 0.95 * v_ref[place] + 0.05 * g * g
        step = m * lax.rsqrt(v + 1e-8) + 0.1 * w
        wo_ref[place] = (w - 0.02 * step).astype(BF)
        mo_ref[place] = m
        vo_ref[place] = v

    for half in range(PANEL // LANES):
        lanes = pl.ds(half * LANES, LANES)

        def body(i, carry):
            here_rows = pl.ds(pl.multiple_of(half * D + i * 128, 128), 128)
            rows = pl.ds(pl.multiple_of(i * 128, 128), 128)
            for j in (1, 2):
                one(j, g_ref[j, here_rows, :].astype(F32) * factor, (rows, lanes))
            return carry

        lax.fori_loop(0, D // 128, body, 0)
        for i in range(D // 128):
            g = g_ref[0, pl.ds(half * D + i * 128, 128), :].astype(F32) * factor
            one(0, g.T, (lanes, pl.ds(i * 128, 128)))


def adamw(total, g, weights):
    wide = pl.BlockSpec((None, D, PANEL), lambda l, p: (l, 0, p))
    tall = pl.BlockSpec((None, PANEL, D), lambda l, p: (l, p, 0))
    specs = [tall] * 3 + [wide] * 6
    arrays = [a for one in weights for a in one]
    return pl.pallas_call(
        adamw_kernel,
        grid=(2, PANELS),
        out_shape=[jax.ShapeDtypeStruct(a.shape, a.dtype) for a in arrays],
        in_specs=[
            pl.BlockSpec((8, LANES), lambda l, p: (0, 0)),
            pl.BlockSpec((3, None, PANEL // LANES * D, LANES), lambda l, p: (0, 1 - l, p, 0)),
            *specs,
        ],
        out_specs=specs,
        scratch_shapes=[pltpu.VMEM((8, LANES), F32)],
        compiler_params=pltpu.CompilerParams(vmem_limit_bytes=LIMIT, dimension_semantics=("arbitrary", "arbitrary")),
        cost_estimate=pl.CostEstimate(flops=6 * D * FF * 30, bytes_accessed=6 * D * FF * 22, transcendentals=6 * D * FF),
        name="adamw",
    )(total, g, *arrays)


def solution(mesh):
    def step(x, dy, w_gate, w_up, w_down, m_gate, m_up, m_down, v_gate, v_up, v_down):
        xt, ys = row_wise(x[0], dy[0], w_gate, w_up, w_down)
        shards, squares = scattered(xt, ys)
        full, total = gathered(shards, squares)
        new = adamw(
            total,
            full.reshape(3, 2, 128 * SHARD, LANES),
            ((w_down, m_down, v_down), (w_gate, m_gate, v_gate), (w_up, m_up, v_up)),
        )
        return tuple(new[3 * j + which] for which in range(3) for j in (1, 2, 0))

    return jax.shard_map(
        step,
        mesh=mesh,
        in_specs=(P(("rep", "dp"), None, None),) * 2 + (P(None, None, None),) * 9,
        out_specs=(P("rep", None, None),) * 9,
        check_vma=False,
    )
```
